256 devices in a mesh: dom: 256 (over z, x, y, core).
Axes of the slice: x: 4, y: 4, z: 8, core: 2. Of those that a mesh axis runs over, the one named last changes fastest.
Arguments:
- entities: float32 [262144, 200], P('dom'), may hold values from -3 to 3
- entity_state: float32 [262144], P('dom'), may hold values from 1e-05 to 0.1
- relations: float32 [1345, 200], replicated, may hold values from -3 to 3
- relation_state: float32 [1345], replicated, may hold values from 1 to 100
- edges: int32 [2, 3, 131072], P(None, None, 'dom'), may hold values from 0 to 1344, as said below
- negatives: int32 [2, 1024, 1000], P(None, 'dom'), may hold values from 0 to 1023
- counts: int32 [2, 256], P(None, 'dom'), may hold values from 1 to 512, as said below
Outputs:
- entities_after: float32 [262144, 200], P('dom')
- entity_state_after: float32 [262144], P('dom')
- relations_after: float32 [1345, 200], replicated
- relation_state_after: float32 [1345], replicated
The draws below stay inside these ranges and needn't reach their ends.
Inputs may be any that keep to these rules, and one draw needn't show every extreme that they name: `edges`: rows 0 and 2 are local entity ids below 1024; row 1 holds relation ids below 1345. `negatives`: local ids in the partner's partition. `counts`: in every round some bucket is full.
All inputs are finite; a program needn't handle non-finite values.
Results may differ from the reference program's by a relative error of at most 0.0003.
Values sent between devices are 32-bit elements; how exact they have to be, the bound alone decides.
No kernel may reach another device: no remote copies, remote signals or barrier semaphores. Data moves between devices by JAX's collectives and lax.ppermute only.
A program may use at most 64 MiB of HBM per device.

```python
import math
import jax
import jax.numpy as jnp
from jax import lax

ENT_DEV = 1024
DIM = 200
REL = 1345
NEG = 1000
BLOCK = 128
BLOCKS = 4
ROUNDS = 2
EDGES_DEV = 512
PARTITIONS = 256
ENTITIES = 262144
TOTAL_EDGES = 131072
ALL_BLOCKS = 1024


def draw_edges(key, part):
    keys = jax.random.split(jax.random.fold_in(key, 11), 4)
    source = jax.random.randint(keys[0], (ROUNDS, 1, TOTAL_EDGES), 0, ENT_DEV, dtype=jnp.int32)
    target = jax.random.randint(keys[1], (ROUNDS, 1, TOTAL_EDGES), 0, ENT_DEV, dtype=jnp.int32)
    first = jax.random.randint(keys[2], (ROUNDS, 1, TOTAL_EDGES), 0, REL, dtype=jnp.int32)
    second = jax.random.randint(keys[3], (ROUNDS, 1, TOTAL_EDGES), 0, REL, dtype=jnp.int32)
    relation = first * second // REL
    return jnp.concatenate([source, relation, target], axis=1).astype(jnp.int32)


def draw_counts(key, part):
    keys = jax.random.split(jax.random.fold_in(key, 23), 3)
    first = jax.random.randint(keys[0], (ROUNDS, PARTITIONS), 0, EDGES_DEV, dtype=jnp.int32)
    second = jax.random.randint(keys[1], (ROUNDS, PARTITIONS), 0, EDGES_DEV, dtype=jnp.int32)
    filled = 1 + first * second // EDGES_DEV
    fullest = jax.random.randint(keys[2], (ROUNDS, 1), 0, PARTITIONS, dtype=jnp.int32)
    places = jnp.arange(PARTITIONS, dtype=jnp.int32)[None, :]
    return jnp.where(places == fullest, EDGES_DEV, filled).astype(jnp.int32)


def set_ends(values, rng, smallest, high):
    extent = values.shape
    place = [jax.random.randint(jax.random.fold_in(rng, axis), (), 0, extent[axis]) for axis in range(len(extent))]
    values = values.at[tuple(place)].set(smallest)
    longest = extent.index(max(extent))
    place[longest] = (place[longest] + 1) % extent[longest]
    return values.at[tuple(place)].set(high)


def shard_levels(key, extent, cuts, smallest, high):
    def one(dim, parts):
        heights = jax.random.uniform(jax.random.fold_in(jax.random.fold_in(key, 6), dim), (parts,), jnp.float32, smallest / len(cuts), high / len(cuts))
        return jnp.repeat(jnp.exp(heights), extent[dim] // parts).reshape((-1,) + (1,) * (len(extent) - dim - 1))

    loudness = one(*cuts[0])
    for cut in cuts[1:]:
        loudness = loudness * one(*cut)
    return loudness


def scatter_about(stream_key, dims, scale, bound, shards=(), kind=jnp.bfloat16):
    drawn = scale * jax.random.normal(stream_key, dims, jnp.float32)
    if shards:
        drawn = drawn * shard_levels(stream_key, dims, shards, -0.22, 0.18)
    return jnp.clip(drawn, -bound, bound).astype(kind)


def setup_inputs(seed: int = 0) -> dict:
    seeds = jax.random.split(jax.random.key(seed), 8)
    return {
        "entities": scatter_about(seeds[0], (ENTITIES, DIM), 0.5, 3.0, ((0, 256),), jnp.float32),
        "entity_state": jnp.clip(jnp.exp(math.log(0.1) - 9.2103404 * jax.random.uniform(seeds[1], (ENTITIES,), jnp.float32) ** shard_levels(seeds[1], (ENTITIES,), ((0, 256),), -0.2, 0.2)), 9.999999747378752e-06, 0.1),
        "relations": scatter_about(seeds[2], (REL, DIM), 0.5, 3.0, (), jnp.float32),
        "relation_state": jnp.clip(jnp.exp(jax.random.uniform(seeds[3], (REL,), jnp.float32, math.log(1.0), math.log(100.0))), 1.0, 100.0),
        "edges": draw_edges(jax.random.fold_in(seeds[7], 71), 0),
        "negatives": set_ends(jax.random.randint(seeds[5], (ROUNDS, ALL_BLOCKS, NEG), 0, ENT_DEV), jax.random.fold_in(seeds[5], 1), 0, ENT_DEV - 1).astype(jnp.int32),
        "counts": draw_counts(jax.random.fold_in(seeds[7], 71), 0),
    }


RATE = 0.2
HIGH = lax.Precision.HIGHEST

def block_terms(carry, table, relations, source, relation, target, negative_ids, live):
    grad_table, grad_relation = carry
    half = table.shape[1] // 2
    src_rows = table[source]
    tgt_rows = table[target]
    neg_rows = table[negative_ids]
    rel_rows = relations[relation]
    src_real, src_imag = (src_rows[:, :half], src_rows[:, half:])
    rel_real, rel_imag = (rel_rows[:, :half], rel_rows[:, half:])
    product = jnp.concatenate([src_real * rel_real - src_imag * rel_imag, src_real * rel_imag + src_imag * rel_real], axis=1)
    positive = lax.optimization_barrier(jnp.sum(product * tgt_rows, axis=1))
    negative = lax.dot_general(product, neg_rows, (((1,), (1,)), ((), ())), precision=HIGH, preferred_element_type=jnp.float32)
    pos_weight = -jax.nn.sigmoid(-positive) * live
    neg_weight = jax.nn.sigmoid(negative) * (live[:, None] / negative.shape[1])
    upstream = pos_weight[:, None] * tgt_rows + jnp.dot(neg_weight, neg_rows, precision=HIGH, preferred_element_type=jnp.float32)
    target_grad = pos_weight[:, None] * product
    negative_grad = lax.dot_general(neg_weight, product, (((0,), (0,)), ((), ())), precision=HIGH, preferred_element_type=jnp.float32)
    up_real, up_imag = (upstream[:, :half], upstream[:, half:])
    source_grad = jnp.concatenate([up_real * rel_real + up_imag * rel_imag, up_imag * rel_real - up_real * rel_imag], axis=1)
    relation_grad = jnp.concatenate([up_real * src_real + up_imag * src_imag, up_imag * src_real - up_real * src_imag], axis=1)
    grad_table = grad_table.at[source].add(source_grad).at[target].add(target_grad).at[negative_ids].add(negative_grad)
    grad_relation = grad_relation.at[relation].add(relation_grad)
    return (grad_table, grad_relation)

def bucket_pass(carry, table, relations, edge_pair, negative_pair, count_pair, source_shift, target_shift, block, first, last):
    block_pair = (count_pair + block - 1) // block

    def visit(index, inner):
        which = (index >= block_pair[0]).astype(jnp.int32)
        number = (index - which * block_pair[0]).astype(jnp.int32)
        edge_list = lax.dynamic_index_in_dim(edge_pair, which, 0, keepdims=False)
        start = (number * block).astype(jnp.int32)
        window = lax.dynamic_slice_in_dim(edge_list, start, block, 1)
        negative_list = lax.dynamic_index_in_dim(negative_pair, which, 0, keepdims=False)
        negative_ids = lax.dynamic_index_in_dim(negative_list, number, 0, keepdims=False) + target_shift[which]
        live = (start + jnp.arange(block, dtype=jnp.int32) < count_pair[which]).astype(jnp.float32)
        return block_terms(inner, table, relations, window[0] + source_shift[which], window[1], window[2] + target_shift[which], negative_ids, live)
    return lax.fori_loop(first, last, visit, carry)

def adagrad(param, state, grad):
    new_state = state + lax.optimization_barrier(jnp.mean(grad * grad, axis=1))
    return (param - RATE * grad / jnp.sqrt(new_state)[:, None], new_state)

def round_pass(entities, entity_state, relations, edge_round, negative_round, count_round, span):
    source_shift = jnp.array([0, ENT_DEV], dtype=jnp.int32)
    target_shift = jnp.array([ENT_DEV, 0], dtype=jnp.int32)

    def visit_pair(pair, carry):
        new_entities, new_state, grad_relation = carry
        pair = pair.astype(jnp.int32)
        lower = (pair // span * (2 * span) + pair % span).astype(jnp.int32)
        upper = (lower + span).astype(jnp.int32)
        low_rows = lax.dynamic_slice_in_dim(entities, (lower * ENT_DEV).astype(jnp.int32), ENT_DEV, 0)
        high_rows = lax.dynamic_slice_in_dim(entities, (upper * ENT_DEV).astype(jnp.int32), ENT_DEV, 0)
        table = jnp.concatenate([low_rows, high_rows], axis=0)
        edge_pair = jnp.stack([lax.dynamic_slice_in_dim(edge_round, (lower * EDGES_DEV).astype(jnp.int32), EDGES_DEV, 1), lax.dynamic_slice_in_dim(edge_round, (upper * EDGES_DEV).astype(jnp.int32), EDGES_DEV, 1)])
        negative_pair = jnp.stack([lax.dynamic_slice_in_dim(negative_round, (lower * BLOCKS).astype(jnp.int32), BLOCKS, 0), lax.dynamic_slice_in_dim(negative_round, (upper * BLOCKS).astype(jnp.int32), BLOCKS, 0)])
        count_pair = jnp.stack([lax.dynamic_index_in_dim(count_round, lower, 0, keepdims=False), lax.dynamic_index_in_dim(count_round, upper, 0, keepdims=False)]).astype(jnp.int32)
        block_pair = (count_pair + BLOCK - 1) // BLOCK
        grads = jnp.zeros((2 * ENT_DEV, DIM), jnp.float32)
        grads, grad_relation = bucket_pass((grads, grad_relation), table, relations, edge_pair, negative_pair, count_pair, source_shift, target_shift, BLOCK, jnp.int32(0), (block_pair[0] + block_pair[1]).astype(jnp.int32))
        for side, which in ((lower, 0), (upper, 1)):
            offset = (side * ENT_DEV).astype(jnp.int32)
            rows = table[which * ENT_DEV:(which + 1) * ENT_DEV]
            state = lax.dynamic_slice_in_dim(entity_state, offset, ENT_DEV, 0)
            rows, state = adagrad(rows, state, grads[which * ENT_DEV:(which + 1) * ENT_DEV])
            new_entities = lax.dynamic_update_slice_in_dim(new_entities, rows, offset, 0)
            new_state = lax.dynamic_update_slice_in_dim(new_state, state, offset, 0)
        return (new_entities, new_state, grad_relation)
    start = (entities, entity_state, jnp.zeros((REL, DIM), jnp.float32))
    new_entities, new_state, grad_relation = lax.fori_loop(jnp.int32(0), jnp.int32(PARTITIONS // 2), visit_pair, start)
    return (new_entities, new_state, grad_relation)

def reference(entities, entity_state, relations, relation_state, edges, negatives, counts):
    levels = PARTITIONS.bit_length() - 1
    for round_index, bit in enumerate((levels - 1, 0)):
        entities, entity_state, grad_relation = round_pass(entities, entity_state, relations, edges[round_index], negatives[round_index], counts[round_index], 2 ** bit)
        relations, relation_state = adagrad(relations, relation_state, grad_relation)
    return (entities, entity_state, relations, relation_state)
```

```python
import functools
import jax
import jax.numpy as jnp
from jax import lax
from jax.experimental import pallas as pl
from jax.experimental.pallas import tpu as pltpu
from jax.sharding import Mesh
from jax.sharding import PartitionSpec as P

Z, X, Y, C = "z", "x", "y", "c"
DOM = (Z, X, Y, C)
F32 = jnp.float32
BF16 = jnp.bfloat16
RATE = 0.2

ROWS = 1024
DIM = 200
HALF = DIM // 2
REL = 1345
RELP = 1408
NEG = 1000
BLOCK = 128
EDGES = 512
LOAD = 216
ID_ROW = 200
HIST_ROW = 208
FLAT = 2304
SIDE = FLAT // 2

VMEM = pl.BlockSpec(memory_space=pltpu.VMEM)
SMEM = pl.BlockSpec(memory_space=pltpu.SMEM)


def shape(*dims, dtype=F32):
    return jax.ShapeDtypeStruct(dims, dtype)


def params():
    return pltpu.CompilerParams(vmem_limit_bytes=48 * 1024 * 1024)


def halves(value):
    high = value.astype(BF16)
    return high, (value - high.astype(F32)).astype(BF16)


def dot(a, b, dims=((1,), (0,))):
    return lax.dot_general(a, b, (dims, ((), ())), preferred_element_type=F32)


NT = ((1,), (1,))


def dot3(a, b, dims=((1,), (0,))):
    return dot(a[0], b[0], dims) + (dot(a[1], b[0], dims) + dot(a[0], b[1], dims))


def one_hot(ids, count):
    places = lax.broadcasted_iota(jnp.int32, (count, ids.shape[1]), 0)
    return jnp.where(places == ids, 1.0, 0.0).astype(BF16)


def histogram(ids):
    upper = lax.broadcasted_iota(jnp.int32, (8, NEG), 0)
    lower = lax.broadcasted_iota(jnp.int32, (128, NEG), 0)
    high = jnp.where(upper == (ids >> 7), 1.0, 0.0).astype(BF16)
    low = jnp.where(lower == (ids & 127), 1.0, 0.0).astype(BF16)
    return dot(high, low, NT)


def live_sources(edges_ref, count, which):
    places = lax.broadcasted_iota(jnp.int32, (1, EDGES), 1)
    return jnp.where(places < count, edges_ref[which, 0:1, :], -1)


def write_payload(out_refs, table, edges_ref, negatives_ref, count, which):
    source = live_sources(edges_ref, count, which)
    pick = one_hot(source, ROWS)
    high, low = halves(table)
    rows = dot(high, pick) + dot(low, pick)
    wide = EDGES // len(out_refs)
    for number, ref in enumerate(out_refs):
        span = slice(number * wide, (number + 1) * wide)
        ref[0:DIM, :] = rows[:, span]
        ref[ID_ROW : ID_ROW + 1, :] = edges_ref[which, 1:2, span].astype(F32)
        ref[ID_ROW + 1 : ID_ROW + 2, :] = edges_ref[which, 2:3, span].astype(F32)
        ref[ID_ROW + 2 : HIST_ROW, :] = jnp.zeros((HIST_ROW - ID_ROW - 2, wide), F32)
        for block in range(wide // BLOCK):
            k = number * (wide // BLOCK) + block
            ref[HIST_ROW:LOAD, block * BLOCK : (block + 1) * BLOCK] = histogram(
                negatives_ref[which, k : k + 1, :]
            )


def prepare(counts_ref, table_ref, edges_ref, negatives_ref, table_out, first, second):
    table = table_ref[...].T
    table_out[...] = table
    write_payload((first, second), table, edges_ref, negatives_ref, counts_ref[0, 0], 0)


def turn_relations(rel_ref, state_ref, rel_out, state_out):
    rel_out[:, 0 : 10 * 128] = rel_ref[0 : 10 * 128, :].T
    last = jnp.concatenate(
        [rel_ref[10 * 128 : REL, :], jnp.zeros((RELP - REL, DIM), F32)], axis=0
    )
    rel_out[:, 10 * 128 : RELP] = last.T
    state_out[...] = jnp.ones((1, RELP), F32)
    state_out[:, 0:REL] = state_ref[...]


def multiply(a_re, a_im, b_re, b_im, conjugate, out):
    if conjugate:
        out[0:HALF, :] = a_re * b_re + a_im * b_im
        out[HALF:DIM, :] = a_im * b_re - a_re * b_im
    else:
        out[0:HALF, :] = a_re * b_re - a_im * b_im
        out[HALF:DIM, :] = a_re * b_im + a_im * b_re


def weights(scores, times, target, first_lane):
    small = jnp.exp(-jnp.abs(scores))
    large = 1.0 / (1.0 + small)
    small = small * large
    up = scores >= 0.0
    plus = jnp.where(up, large, small)
    minus = jnp.where(up, small, large)
    lanes = lax.broadcasted_iota(jnp.int32, (1, 128), 1) + first_lane
    return plus * times - jnp.where(lanes == target, minus, 0.0)


def edge_terms(load_ref, table, relations, work, outs, carried):
    s_ref, w_ref, q_ref, score_ref, high_ref, low_ref, back_ref, rg_ref = work
    sg_out, table_grad = outs
    wide = load_ref.shape[1]
    pick = one_hot(load_ref[ID_ROW : ID_ROW + 1, :].astype(jnp.int32), RELP)
    rel_high, rel_low = halves(relations)
    w_ref[...] = dot(rel_high, pick) + dot(rel_low, pick)
    s_re, s_im = load_ref[0:HALF, :], load_ref[HALF:DIM, :]
    w_re, w_im = w_ref[0:HALF, :], w_ref[HALF:DIM, :]
    multiply(s_re, s_im, w_re, w_im, False, q_ref)
    product = q_ref[...]
    table_parts = halves(table)
    score_ref[...] = dot3(halves(product.T), table_parts)
    target = load_ref[ID_ROW : ID_ROW + 8, :].T[:, 1:2].astype(jnp.int32)
    for block in range(wide // BLOCK):
        edges = slice(block * BLOCK, (block + 1) * BLOCK)
        for tile in range(ROWS // 128):
            lanes = slice(tile * 128, (tile + 1) * 128)
            times = load_ref[HIST_ROW + tile : HIST_ROW + tile + 1, edges] * (1.0 / NEG)
            value = weights(score_ref[edges, lanes], times, target[edges], tile * 128)
            high_ref[edges, lanes], low_ref[edges, lanes] = halves(value)
    weight_parts = high_ref[...], low_ref[...]
    back_ref[...] = dot3(table_parts, weight_parts, NT)
    grad = dot3(halves(product), weight_parts)
    table_grad[...] = grad if carried is None else grad + carried[0][...]
    up_re, up_im = back_ref[0:HALF, :], back_ref[HALF:DIM, :]
    multiply(up_re, up_im, w_re, w_im, True, sg_out)
    multiply(up_re, up_im, s_re, s_im, True, rg_ref)
    rg_high, rg_low = halves(rg_ref[...])
    grad = dot(rg_high, pick, NT) + dot(rg_low, pick, NT)
    return grad if carried is None else grad + carried[1][...]


def split_flat(core, grad, flat, send_out, keep_out):
    for tile in range(RELP // 128):
        flat[tile * DIM : (tile + 1) * DIM, :] = grad[:, tile * 128 : (tile + 1) * 128]
    flat[RELP // 128 * DIM : FLAT, :] = jnp.zeros((FLAT - RELP // 128 * DIM, 128), F32)
    keep_out[...] = flat[pl.ds(pl.multiple_of(core * SIDE, SIDE), SIDE), :]
    send_out[...] = flat[pl.ds(pl.multiple_of((1 - core) * SIDE, SIDE), SIDE), :]


def join_flat(core, mine_ref, other_ref, flat):
    flat[pl.ds(pl.multiple_of(core * SIDE, SIDE), SIDE), :] = mine_ref[...]
    flat[pl.ds(pl.multiple_of((1 - core) * SIDE, SIDE), SIDE), :] = other_ref[...]


def adagrad(table, state, grad):
    state = state + jnp.sum(grad * grad, axis=0, keepdims=True) * (1.0 / DIM)
    return table - grad * (RATE / jnp.sqrt(state)), state


def first_piece(load_ref, table_ref, rel_ref, sg_out, table_grad, rel_grad, *work):
    rel_grad[...] = edge_terms(
        load_ref, table_ref[...], rel_ref[...], work, (sg_out, table_grad), None
    )


def second_piece(
    core_ref, load_ref, table_ref, rel_ref, g_ref, h_ref, sg_out, table_grad, send, keep, *work
):
    grad = edge_terms(
        load_ref, table_ref[...], rel_ref[...], work[:-1], (sg_out, table_grad), (g_ref, h_ref)
    )
    split_flat(core_ref[0], grad, work[-1], send, keep)


def step_relations(core, mine_ref, other_ref, rel_ref, state_ref, flat, rel_out, state_out):
    join_flat(core, mine_ref, other_ref, flat)
    for tile in range(RELP // 128):
        lanes = slice(tile * 128, (tile + 1) * 128)
        rel_out[:, lanes], state_out[:, lanes] = adagrad(
            rel_ref[:, lanes], state_ref[:, lanes], flat[tile * DIM : (tile + 1) * DIM, :]
        )


def second_round(
    core_ref,
    mine_ref,
    other_ref,
    rel_ref,
    state_ref,
    load_ref,
    table_ref,
    sg_out,
    table_grad,
    send,
    keep,
    rel_out,
    state_out,
    *work,
):
    core, flat = core_ref[0], work[-1]
    step_relations(core, mine_ref, other_ref, rel_ref, state_ref, flat, rel_out, state_out)
    grad = edge_terms(
        load_ref, table_ref[...], rel_out[...], work[:-1], (sg_out, table_grad), None
    )
    split_flat(core, grad, flat, send, keep)


def step_entities(table_ref, state_ref, grad_ref, back_refs, edges_ref, count, which):
    pick = one_hot(live_sources(edges_ref, count, which), ROWS)
    grad = grad_ref[...]
    wide = EDGES // len(back_refs)
    for number, ref in enumerate(back_refs):
        high, low = halves(ref[...])
        part = pick[:, number * wide : (number + 1) * wide]
        grad = grad + (dot(high, part, NT) + dot(low, part, NT))
    return adagrad(table_ref[...], state_ref[...], grad)


def between(
    counts_ref,
    table_ref,
    state_ref,
    grad_ref,
    back_a,
    back_b,
    edges_ref,
    negatives_ref,
    table_out,
    state_out,
    load,
):
    table, state = step_entities(
        table_ref, state_ref, grad_ref, (back_a, back_b), edges_ref, counts_ref[0, 0], 0
    )
    table_out[...] = table
    state_out[...] = state
    write_payload((load,), table, edges_ref, negatives_ref, counts_ref[1, 0], 1)


def last_entities(
    counts_ref, table_ref, state_ref, grad_ref, back_ref, edges_ref, table_out, state_out
):
    table, state = step_entities(
        table_ref, state_ref, grad_ref, (back_ref,), edges_ref, counts_ref[1, 0], 1
    )
    table_out[...] = table.T
    state_out[...] = state


def last_relations(
    core_ref, mine_ref, other_ref, rel_ref, state_ref, rel_out, state_out, flat, rel, state
):
    step_relations(core_ref[0], mine_ref, other_ref, rel_ref, state_ref, flat, rel, state)
    rel_out[0 : 10 * 128, :] = rel[:, 0 : 10 * 128].T
    rel_out[10 * 128 : REL, :] = rel[:, 10 * 128 : RELP].T[0 : REL - 10 * 128, :]
    state_out[...] = state[:, 0:REL]


def work_shapes(wide):
    return [
        pltpu.VMEM((DIM, wide), F32),
        pltpu.VMEM((DIM, wide), F32),
        pltpu.VMEM((DIM, wide), F32),
        pltpu.VMEM((wide, ROWS), F32),
        pltpu.VMEM((wide, ROWS), BF16),
        pltpu.VMEM((wide, ROWS), BF16),
        pltpu.VMEM((DIM, wide), F32),
        pltpu.VMEM((DIM, wide), F32),
    ]


def call(body, ins, outs, operands, scratch=(), flops=0):
    specs = [SMEM if kind else VMEM for kind in ins]
    return pl.pallas_call(
        body,
        out_shape=outs,
        in_specs=specs,
        out_specs=[VMEM] * len(outs),
        scratch_shapes=list(scratch),
        compiler_params=params(),
        cost_estimate=pl.CostEstimate(flops=flops, bytes_accessed=0, transcendentals=0),
        name=body.__name__,
    )(*operands)


def across(value, axis, apart):
    count = lax.axis_size(axis)
    return lax.ppermute(value, axis, [(i, i ^ apart) for i in range(count)])


def total(send, keep):
    part = (keep + across(send, C, 1)).reshape(16, SIDE // 16, 128)
    part = lax.all_to_all(part, (X, Y), 0, 0, tiled=True).sum(axis=0)
    part = lax.all_to_all(part.reshape(8, SIDE // 128, 128), Z, 0, 0, tiled=True).sum(axis=0)
    part = lax.all_to_all(jnp.broadcast_to(part[None], (8, *part.shape)), Z, 0, 0, tiled=True)
    part = part.reshape(1, SIDE // 16, 128)
    part = lax.all_to_all(jnp.broadcast_to(part, (16, *part.shape[1:])), (X, Y), 0, 0, tiled=True)
    mine = part.reshape(SIDE, 128)
    return mine, across(mine, C, 1)


def body(entities, entity_state, relations, relation_state, edges, negatives, counts):
    core = lax.axis_index(C).astype(jnp.int32).reshape(1)
    state = entity_state.reshape(1, ROWS)
    table, first, second = call(
        prepare,
        (1, 0, 0, 0),
        [shape(DIM, ROWS), shape(LOAD, EDGES // 2), shape(LOAD, EDGES // 2)],
        (counts, entities, edges, negatives),
    )
    first = across(first, Z, 4)
    second = across(second, Z, 4)
    rel, rel_state = call(
        turn_relations,
        (0, 0),
        [shape(DIM, RELP), shape(1, RELP)],
        (relations, relation_state.reshape(1, REL)),
    )
    piece = shape(DIM, EDGES // 2)
    back_a, grad, rel_grad = call(
        first_piece,
        (0, 0, 0),
        [piece, shape(DIM, ROWS), shape(DIM, RELP)],
        (first, table, rel),
        work_shapes(EDGES // 2),
    )
    back_b, grad, send, keep = call(
        second_piece,
        (1, 0, 0, 0, 0, 0),
        [piece, shape(DIM, ROWS), shape(SIDE, 128), shape(SIDE, 128)],
        (core, second, table, rel, grad, rel_grad),
        work_shapes(EDGES // 2) + [pltpu.VMEM((FLAT, 128), F32)],
    )
    back_a = across(back_a, Z, 4)
    back_b = across(back_b, Z, 4)
    mine, other = total(send, keep)
    table, state, load = call(
        between,
        (1, 0, 0, 0, 0, 0, 0, 0),
        [shape(DIM, ROWS), shape(1, ROWS), shape(LOAD, EDGES)],
        (counts, table, state, grad, back_a, back_b, edges, negatives),
    )
    load = across(load, C, 1)
    back, grad, send, keep, rel, rel_state = call(
        second_round,
        (1, 0, 0, 0, 0, 0, 0),
        [
            shape(DIM, EDGES),
            shape(DIM, ROWS),
            shape(SIDE, 128),
            shape(SIDE, 128),
            shape(DIM, RELP),
            shape(1, RELP),
        ],
        (core, mine, other, rel, rel_state, load, table),
        work_shapes(EDGES) + [pltpu.VMEM((FLAT, 128), F32)],
    )
    back = across(back, C, 1)
    mine, other = total(send, keep)
    entities, state = call(
        last_entities,
        (1, 0, 0, 0, 0, 0),
        [shape(ROWS, DIM), shape(1, ROWS)],
        (counts, table, state, grad, back, edges),
    )
    relations, rel_state = call(
        last_relations,
        (1, 0, 0, 0, 0),
        [shape(REL, DIM), shape(1, REL)],
        (core, mine, other, rel, rel_state),
        [pltpu.VMEM((FLAT, 128), F32), pltpu.VMEM((DIM, RELP), F32), pltpu.VMEM((1, RELP), F32)],
    )
    return entities, state.reshape(ROWS), relations, rel_state.reshape(REL)


def solution(mesh):
    finer = Mesh(mesh.devices.reshape(8, 4, 4, 2), DOM)
    return jax.shard_map(
        body,
        mesh=finer,
        in_specs=(
            P(DOM, None),
            P(DOM),
            P(),
            P(),
            P(None, None, DOM),
            P(None, DOM, None),
            P(None, DOM),
        ),
        out_specs=(P(DOM, None), P(DOM), P(), P()),
        check_vma=False,
    )
```

```python
import jax
import jax.numpy as jnp
from jax import lax
from jax.experimental import pallas as pl
from jax.experimental.pallas import tpu as pltpu
from jax.sharding import Mesh
from jax.sharding import PartitionSpec as P

Z, X, Y, C = "z", "x", "y", "c"
DOM = (Z, X, Y, C)
F32 = jnp.float32
BF16 = jnp.bfloat16
RATE = 0.2

ROWS = 1024
DIM = 200
HALF = DIM // 2
REL = 1345
RELP = 1408
NEG = 1000
BLOCK = 128
STEP = 256
EDGES = 512
LOAD = 216
ID_ROW = 200
HIST_ROW = 208
FLAT = 2304
SIDE = FLAT // 2

VMEM = pl.BlockSpec(memory_space=pltpu.VMEM)
SMEM = pl.BlockSpec(memory_space=pltpu.SMEM)


def shape(*dims, dtype=F32):
    return jax.ShapeDtypeStruct(dims, dtype)


def params():
    return pltpu.CompilerParams(vmem_limit_bytes=48 * 1024 * 1024)


def halves(value):
    high = value.astype(BF16)
    return high, (value - high.astype(F32)).astype(BF16)


def dot(a, b, dims=((1,), (0,))):
    return lax.dot_general(a, b, (dims, ((), ())), preferred_element_type=F32)


NT = ((1,), (1,))


def dot3(a, b, dims=((1,), (0,))):
    return dot(a[0], b[0], dims) + (dot(a[1], b[0], dims) + dot(a[0], b[1], dims))


def one_hot(ids, count):
    places = lax.broadcasted_iota(jnp.int32, (count, ids.shape[1]), 0)
    return jnp.where(places == ids, 1.0, 0.0).astype(BF16)


def histogram(ids):
    upper = lax.broadcasted_iota(jnp.int32, (8, NEG), 0)
    lower = lax.broadcasted_iota(jnp.int32, (128, NEG), 0)
    high = jnp.where(upper == (ids >> 7), 1.0, 0.0).astype(BF16)
    low = jnp.where(lower == (ids & 127), 1.0, 0.0).astype(BF16)
    return dot(high, low, NT)


def live_sources(edges_ref, count, which):
    places = lax.broadcasted_iota(jnp.int32, (1, EDGES), 1)
    return jnp.where(places < count, edges_ref[which, 0:1, :], -1)


def write_payload(out_refs, parts, edges_ref, negatives_ref, count, which):
    source = live_sources(edges_ref, count, which)
    pick = one_hot(source, ROWS)
    high, low = parts
    rows = dot(high, pick) + dot(low, pick)
    wide = EDGES // len(out_refs)
    for number, ref in enumerate(out_refs):
        span = slice(number * wide, (number + 1) * wide)
        ref[0:DIM, :] = rows[:, span]
        ref[ID_ROW : ID_ROW + 1, :] = edges_ref[which, 1:2, span].astype(F32)
        ref[ID_ROW + 1 : ID_ROW + 2, :] = edges_ref[which, 2:3, span].astype(F32)
        ref[ID_ROW + 2 : HIST_ROW, :] = jnp.zeros((HIST_ROW - ID_ROW - 2, wide), F32)
        for block in range(wide // BLOCK):
            k = number * (wide // BLOCK) + block
            ref[HIST_ROW:LOAD, block * BLOCK : (block + 1) * BLOCK] = histogram(
                negatives_ref[which, k : k + 1, :]
            )


def prepare(counts_ref, table_ref, edges_ref, negatives_ref, high_out, low_out, first, second):
    parts = halves(table_ref[...])
    high_out[...], low_out[...] = parts
    write_payload((first, second), parts, edges_ref, negatives_ref, counts_ref[0, 0], 0)


def pad_relations(rel_ref, state_ref, rel_out, state_out, high_out, low_out):
    rel_out[:, 10 * 128 : RELP] = jnp.zeros((DIM, RELP - 10 * 128), F32)
    rel_out[:, 0:REL] = rel_ref[...]
    high_out[...], low_out[...] = halves(rel_out[...])
    state_out[...] = jnp.ones((1, RELP), F32)
    state_out[:, 0:REL] = state_ref[...]


def multiply(a_re, a_im, b_re, b_im, conjugate, out, lanes):
    if conjugate:
        out[0:HALF, lanes] = a_re * b_re + a_im * b_im
        out[HALF:DIM, lanes] = a_im * b_re - a_re * b_im
    else:
        out[0:HALF, lanes] = a_re * b_re - a_im * b_im
        out[HALF:DIM, lanes] = a_re * b_im + a_im * b_re


def weights(scores, times, target, first_lane):
    small = jnp.exp(-jnp.abs(scores))
    large = 1.0 / (1.0 + small)
    small = small * large
    up = scores >= 0.0
    plus = jnp.where(up, large, small)
    minus = jnp.where(up, small, large)
    lanes = lax.broadcasted_iota(jnp.int32, (1, 128), 1) + first_lane
    return plus * times - jnp.where(lanes == target, minus, 0.0)


def edge_terms(load_ref, table_parts, rel_parts, work, sg_out, first, carried):
    w_ref, q_ref, score_ref, high_ref, low_ref, back_ref, rg_ref = work
    wide = load_ref.shape[1]
    pick = one_hot(load_ref[ID_ROW : ID_ROW + 1, :].astype(jnp.int32), RELP)
    w_ref[...] = dot(rel_parts[0], pick) + dot(rel_parts[1], pick)
    s_re, s_im = load_ref[0:HALF, :], load_ref[HALF:DIM, :]
    w_re, w_im = w_ref[0:HALF, :], w_ref[HALF:DIM, :]
    multiply(s_re, s_im, w_re, w_im, False, q_ref, slice(None))
    product = q_ref[...]
    product_parts = halves(product)
    target = load_ref[ID_ROW : ID_ROW + 8, :].T[:, 1:2].astype(jnp.int32)
    turned = halves(product.T)
    for start in range(0, wide, STEP):
        edges = slice(start, start + STEP)
        score_ref[edges, :] = dot3((turned[0][edges], turned[1][edges]), table_parts)
    table_grad = None
    for start in range(0, wide, STEP):
        for block in range(start, start + STEP, BLOCK):
            edges = slice(block, block + BLOCK)
            for tile in range(ROWS // 128):
                lanes = slice(tile * 128, (tile + 1) * 128)
                times = load_ref[HIST_ROW + tile : HIST_ROW + tile + 1, edges] * (1.0 / NEG)
                value = weights(score_ref[edges, lanes], times, target[edges], tile * 128)
                high_ref[edges, lanes], low_ref[edges, lanes] = halves(value)
        edges = slice(start, start + STEP)
        weight_parts = high_ref[edges, :], low_ref[edges, :]
        back_ref[:, edges] = dot3(table_parts, weight_parts, NT)
        part = dot3((product_parts[0][:, edges], product_parts[1][:, edges]), weight_parts)
        table_grad = part if table_grad is None else table_grad + part
    if carried is not None:
        table_grad = table_grad + carried[0][...]
    up_re, up_im = back_ref[0:HALF, :], back_ref[HALF:DIM, :]
    multiply(up_re, up_im, s_re, s_im, True, rg_ref, slice(None))
    multiply(up_re, up_im, w_re, w_im, True, sg_out, slice(first, first + wide))
    rg_high, rg_low = halves(rg_ref[...])
    grad = dot(rg_high, pick, NT) + dot(rg_low, pick, NT)
    return table_grad, grad if carried is None else grad + carried[1][...]


def split_flat(core, grad, flat, send_out, keep_out):
    for tile in range(RELP // 128):
        flat[tile * DIM : (tile + 1) * DIM, :] = grad[:, tile * 128 : (tile + 1) * 128]
    flat[RELP // 128 * DIM : FLAT, :] = jnp.zeros((FLAT - RELP // 128 * DIM, 128), F32)
    keep_out[...] = flat[pl.ds(pl.multiple_of(core * SIDE, SIDE), SIDE), :]
    send_out[...] = flat[pl.ds(pl.multiple_of((1 - core) * SIDE, SIDE), SIDE), :]


def join_flat(core, mine_ref, other_ref, flat):
    flat[pl.ds(pl.multiple_of(core * SIDE, SIDE), SIDE), :] = mine_ref[...]
    flat[pl.ds(pl.multiple_of((1 - core) * SIDE, SIDE), SIDE), :] = other_ref[...]


def adagrad(table, state, grad):
    state = state + jnp.sum(grad * grad, axis=0, keepdims=True) * (1.0 / DIM)
    return table - grad * (RATE / jnp.sqrt(state)), state


def first_piece(
    load_ref, high_ref, low_ref, rel_high, rel_low, sg_out, table_grad, rel_grad, *work
):
    table_parts, rel_parts = (high_ref[...], low_ref[...]), (rel_high[...], rel_low[...])
    table_grad[...], rel_grad[...] = edge_terms(
        load_ref, table_parts, rel_parts, work, sg_out, 0, None
    )


def second_piece(
    core_ref,
    load_ref,
    high_ref,
    low_ref,
    rel_high,
    rel_low,
    sg_ref,
    g_ref,
    h_ref,
    sg_out,
    table_grad,
    send,
    keep,
    *work,
):
    table_parts, rel_parts = (high_ref[...], low_ref[...]), (rel_high[...], rel_low[...])
    first = sg_ref.shape[1]
    sg_out[:, 0:first] = sg_ref[...]
    table_grad[...], grad = edge_terms(
        load_ref, table_parts, rel_parts, work[:-1], sg_out, first, (g_ref, h_ref)
    )
    split_flat(core_ref[0], grad, work[-1], send, keep)


def step_relations(core, mine_ref, other_ref, rel_ref, state_ref, flat, rel_out, state_out):
    join_flat(core, mine_ref, other_ref, flat)
    for tile in range(RELP // 128):
        lanes = slice(tile * 128, (tile + 1) * 128)
        rel_out[:, lanes], state_out[:, lanes] = adagrad(
            rel_ref[:, lanes], state_ref[:, lanes], flat[tile * DIM : (tile + 1) * DIM, :]
        )


def second_round(
    core_ref,
    mine_ref,
    other_ref,
    rel_ref,
    state_ref,
    load_ref,
    high_ref,
    low_ref,
    sg_out,
    table_grad,
    send,
    keep,
    rel_out,
    state_out,
    *work,
):
    core, flat = core_ref[0], work[-1]
    step_relations(core, mine_ref, other_ref, rel_ref, state_ref, flat, rel_out, state_out)
    table_grad[...], grad = edge_terms(
        load_ref,
        (high_ref[...], low_ref[...]),
        halves(rel_out[...]),
        work[:-1],
        sg_out,
        0,
        None,
    )
    split_flat(core, grad, flat, send, keep)


def step_entities(table_ref, state_ref, grad_ref, back_ref, edges_ref, count, which):
    pick = one_hot(live_sources(edges_ref, count, which), ROWS)
    high, low = halves(back_ref[...])
    grad = grad_ref[...] + (dot(high, pick, NT) + dot(low, pick, NT))
    return adagrad(table_ref[...], state_ref[...], grad)


def between(
    counts_ref,
    table_ref,
    state_ref,
    grad_ref,
    back_ref,
    edges_ref,
    negatives_ref,
    table_out,
    state_out,
    high_out,
    low_out,
    load,
):
    table, state_out[...] = step_entities(
        table_ref, state_ref, grad_ref, back_ref, edges_ref, counts_ref[0, 0], 0
    )
    table_out[...] = table
    parts = halves(table)
    high_out[...], low_out[...] = parts
    write_payload((load,), parts, edges_ref, negatives_ref, counts_ref[1, 0], 1)


def last_entities(
    counts_ref, table_ref, state_ref, grad_ref, back_ref, edges_ref, table_out, state_out
):
    table_out[...], state_out[...] = step_entities(
        table_ref, state_ref, grad_ref, back_ref, edges_ref, counts_ref[1, 0], 1
    )


def last_relations(
    core_ref, mine_ref, other_ref, rel_ref, state_ref, rel_out, state_out, flat, rel, state
):
    step_relations(core_ref[0], mine_ref, other_ref, rel_ref, state_ref, flat, rel, state)
    rel_out[...] = rel[:, 0:REL]
    state_out[...] = state[:, 0:REL]


def work_shapes(wide):
    return [
        pltpu.VMEM((DIM, wide), F32),
        pltpu.VMEM((DIM, wide), F32),
        pltpu.VMEM((wide, ROWS), F32),
        pltpu.VMEM((wide, ROWS), BF16),
        pltpu.VMEM((wide, ROWS), BF16),
        pltpu.VMEM((DIM, wide), F32),
        pltpu.VMEM((DIM, wide), F32),
    ]


def call(body, ins, outs, operands, scratch=(), flops=0):
    specs = [SMEM if kind else VMEM for kind in ins]
    return pl.pallas_call(
        body,
        out_shape=outs,
        in_specs=specs,
        out_specs=[VMEM] * len(outs),
        scratch_shapes=list(scratch),
        compiler_params=params(),
        cost_estimate=pl.CostEstimate(flops=flops, bytes_accessed=0, transcendentals=0),
    )(*operands)


def across(value, axis, apart):
    count = lax.axis_size(axis)
    return lax.ppermute(value, axis, [(i, i ^ apart) for i in range(count)])


def total(send, keep):
    part = (keep + across(send, C, 1)).reshape(16, SIDE // 16, 128)
    part = lax.all_to_all(part, (X, Y), 0, 0, tiled=True).sum(axis=0)
    part = jnp.broadcast_to(part[None], (8, *part.shape))
    part = lax.all_to_all(part, Z, 0, 0, tiled=True).sum(axis=0)
    part = jnp.broadcast_to(part[None], (16, *part.shape))
    part = lax.all_to_all(part, (X, Y), 0, 0, tiled=True)
    mine = part.reshape(SIDE, 128)
    return mine, across(mine, C, 1)


def body(entities, entity_state, relations, relation_state, edges, negatives, counts):
    core = lax.axis_index(C).astype(jnp.int32).reshape(1)
    table, rel = entities.T, relations.T
    state = entity_state.reshape(1, ROWS)
    piece = shape(LOAD, EDGES // 2)
    narrow = shape(DIM, ROWS, dtype=BF16)
    high, low, first, second = call(
        prepare,
        (1, 0, 0, 0),
        [narrow, narrow, piece, piece],
        (counts, table, edges, negatives),
    )
    first = across(first, Z, 4)
    second = across(second, Z, 4)
    wide_rel = shape(DIM, RELP, dtype=BF16)
    rel, rel_state, rel_high, rel_low = call(
        pad_relations,
        (0, 0),
        [shape(DIM, RELP), shape(1, RELP), wide_rel, wide_rel],
        (rel, relation_state.reshape(1, REL)),
    )
    back, grad, rel_grad = call(
        first_piece,
        (0, 0, 0, 0, 0),
        [shape(DIM, EDGES // 2), shape(DIM, ROWS), shape(DIM, RELP)],
        (first, high, low, rel_high, rel_low),
        work_shapes(EDGES // 2),
    )
    back, grad, send, keep = call(
        second_piece,
        (1, 0, 0, 0, 0, 0, 0, 0, 0),
        [shape(DIM, EDGES), shape(DIM, ROWS), shape(SIDE, 128), shape(SIDE, 128)],
        (core, second, high, low, rel_high, rel_low, back, grad, rel_grad),
        work_shapes(EDGES // 2) + [pltpu.VMEM((FLAT, 128), F32)],
    )
    back = across(back, Z, 4)
    mine, other = total(send, keep)
    table, state, high, low, load = call(
        between,
        (1, 0, 0, 0, 0, 0, 0),
        [shape(DIM, ROWS), shape(1, ROWS), narrow, narrow, shape(LOAD, EDGES)],
        (counts, table, state, grad, back, edges, negatives),
    )
    load = across(load, C, 1)
    back, grad, send, keep, rel, rel_state = call(
        second_round,
        (1, 0, 0, 0, 0, 0, 0, 0),
        [
            shape(DIM, EDGES),
            shape(DIM, ROWS),
            shape(SIDE, 128),
            shape(SIDE, 128),
            shape(DIM, RELP),
            shape(1, RELP),
        ],
        (core, mine, other, rel, rel_state, load, high, low),
        work_shapes(EDGES) + [pltpu.VMEM((FLAT, 128), F32)],
    )
    back = across(back, C, 1)
    mine, other = total(send, keep)
    table, state = call(
        last_entities,
        (1, 0, 0, 0, 0, 0),
        [shape(DIM, ROWS), shape(1, ROWS)],
        (counts, table, state, grad, back, edges),
    )
    rel, rel_state = call(
        last_relations,
        (1, 0, 0, 0, 0),
        [shape(DIM, REL), shape(1, REL)],
        (core, mine, other, rel, rel_state),
        [pltpu.VMEM((FLAT, 128), F32), pltpu.VMEM((DIM, RELP), F32), pltpu.VMEM((1, RELP), F32)],
    )
    return table.T, state.reshape(ROWS), rel.T, rel_state.reshape(REL)


def solution(mesh):
    finer = Mesh(mesh.devices.reshape(8, 4, 4, 2), DOM)
    return jax.shard_map(
        body,
        mesh=finer,
        in_specs=(
            P(DOM, None),
            P(DOM),
            P(),
            P(),
            P(None, None, DOM),
            P(None, DOM, None),
            P(None, DOM),
        ),
        out_specs=(P(DOM, None), P(DOM), P(), P()),
        check_vma=False,
    )
```

```python
import jax
import jax.numpy as jnp
from jax import lax
from jax.experimental import pallas as pl
from jax.experimental.pallas import tpu as pltpu
from jax.sharding import Mesh
from jax.sharding import PartitionSpec as P

Z, X, Y, C = "z", "x", "y", "c"
DOM = (Z, X, Y, C)
F32 = jnp.float32
BF16 = jnp.bfloat16
RATE = 0.2

ROWS = 1024
DIM = 200
HALF = DIM // 2
REL = 1345
RELP = 1408
NEG = 1000
BLOCK = 128
STEP = 256
EARLY = 384
EDGES = 512
LOAD = 216
ID_ROW = 200
HIST_ROW = 208
FLAT = 2304
SIDE = FLAT // 2

VMEM = pl.BlockSpec(memory_space=pltpu.VMEM)
SMEM = pl.BlockSpec(memory_space=pltpu.SMEM)
HBM = pl.BlockSpec(memory_space=pltpu.HBM)


def shape(*dims, dtype=F32):
    return jax.ShapeDtypeStruct(dims, dtype)


def params(grant):
    return pltpu.CompilerParams(vmem_limit_bytes=grant)


def halves(value):
    high = value.astype(BF16)
    return high, (value - high.astype(F32)).astype(BF16)


def dot(a, b, dims=((1,), (0,))):
    return lax.dot_general(a, b, (dims, ((), ())), preferred_element_type=F32)


NT = ((1,), (1,))


def dot3(a, b, dims=((1,), (0,))):
    return dot(a[0], b[0], dims) + (dot(a[1], b[0], dims) + dot(a[0], b[1], dims))


def one_hot(ids, count):
    places = lax.broadcasted_iota(jnp.int32, (count, ids.shape[1]), 0)
    return jnp.where(places == ids, 1.0, 0.0).astype(BF16)


def histogram(ids):
    upper = lax.broadcasted_iota(jnp.int32, (8, NEG), 0)
    lower = lax.broadcasted_iota(jnp.int32, (128, NEG), 0)
    high = jnp.where(upper == (ids >> 7), 1.0, 0.0).astype(BF16)
    low = jnp.where(lower == (ids & 127), 1.0, 0.0).astype(BF16)
    return dot(high, low, NT)


def live_sources(edges_ref, count, which):
    places = lax.broadcasted_iota(jnp.int32, (1, EDGES), 1)
    return jnp.where(places < count, edges_ref[0, which : which + 1, :], -1)


def fetch(sem, *pairs):
    copies = [pltpu.make_async_copy(a, b, sem.at[i]) for i, (a, b) in enumerate(pairs)]
    for copy in copies:
        copy.start()
    return copies


def write_payload(out_refs, parts, edges_ref, negatives_ref, count, which):
    source = live_sources(edges_ref, count, which)
    pick = one_hot(source, ROWS)
    high, low = parts
    rows = dot(high, pick) + dot(low, pick)
    first = 0
    for ref in out_refs:
        wide = ref.shape[1]
        span = slice(first, first + wide)
        ref[0:DIM, :] = rows[:, span]
        ref[ID_ROW : ID_ROW + 1, :] = edges_ref[1, which : which + 1, span].astype(F32)
        ref[ID_ROW + 1 : ID_ROW + 2, :] = edges_ref[2, which : which + 1, span].astype(F32)
        ref[ID_ROW + 2 : HIST_ROW, :] = jnp.zeros((HIST_ROW - ID_ROW - 2, wide), F32)
        for block in range(wide // BLOCK):
            k = first // BLOCK + block
            ref[HIST_ROW:LOAD, block * BLOCK : (block + 1) * BLOCK] = histogram(
                negatives_ref[which, k : k + 1, :]
            )
        first += wide


def prepare(
    counts_ref,
    table_hbm,
    edges_hbm,
    negatives_hbm,
    high_out,
    low_out,
    first_out,
    second_out,
    table_ref,
    edges_ref,
    negatives_ref,
    high_ref,
    low_ref,
    first_ref,
    second_ref,
    sem,
):
    copies = fetch(
        sem, (edges_hbm, edges_ref), (table_hbm, table_ref), (negatives_hbm, negatives_ref)
    )
    for copy in copies:
        copy.wait()
    parts = halves(table_ref[...])
    high_ref[...], low_ref[...] = parts
    copies = fetch(sem, (high_ref, high_out), (low_ref, low_out))
    pieces = (first_ref, second_ref)
    write_payload(pieces, parts, edges_ref, negatives_ref, counts_ref[0, 0], 0)
    copies += fetch(sem.at[2:4], (first_ref, first_out), (second_ref, second_out))
    for copy in copies:
        copy.wait()


def pad_relations(rel_ref, state_ref, rel_out, state_out, high_out, low_out):
    rel_out[:, 10 * 128 : RELP] = jnp.zeros((DIM, RELP - 10 * 128), F32)
    rel_out[:, 0:REL] = rel_ref[...]
    high_out[...], low_out[...] = halves(rel_out[...])
    state_out[...] = jnp.ones((1, RELP), F32)
    state_out[:, 0:REL] = state_ref[...]


def multiply(a_re, a_im, b_re, b_im, conjugate, out, lanes):
    if conjugate:
        out[0:HALF, lanes] = a_re * b_re + a_im * b_im
        out[HALF:DIM, lanes] = a_im * b_re - a_re * b_im
    else:
        out[0:HALF, lanes] = a_re * b_re - a_im * b_im
        out[HALF:DIM, lanes] = a_re * b_im + a_im * b_re


def weights(scores, times, target, first_lane):
    small = jnp.exp(-jnp.abs(scores))
    large = 1.0 / (1.0 + small)
    small = small * large
    up = scores >= 0.0
    plus = jnp.where(up, large, small)
    minus = jnp.where(up, small, large)
    lanes = lax.broadcasted_iota(jnp.int32, (1, 128), 1) + first_lane
    return plus * times - jnp.where(lanes == target, minus, 0.0)


def edge_terms(load_ref, table_parts, rel_parts, work, sg_out, rg_ref, first):
    w_ref, q_ref, score_ref, high_ref, low_ref, back_ref = work
    wide = load_ref.shape[1]
    pick = one_hot(load_ref[ID_ROW : ID_ROW + 1, :].astype(jnp.int32), RELP)
    w_ref[...] = dot(rel_parts[0], pick) + dot(rel_parts[1], pick)
    s_re, s_im = load_ref[0:HALF, :], load_ref[HALF:DIM, :]
    w_re, w_im = w_ref[0:HALF, :], w_ref[HALF:DIM, :]
    multiply(s_re, s_im, w_re, w_im, False, q_ref, slice(None))
    product = q_ref[...]
    product_parts = halves(product)
    target = load_ref[ID_ROW : ID_ROW + 8, :].T[:, 1:2].astype(jnp.int32)
    turned = halves(product.T)
    spans = [slice(start, min(start + STEP, wide)) for start in range(0, wide, STEP)]
    for edges in spans:
        score_ref[edges, :] = dot3((turned[0][edges], turned[1][edges]), table_parts)
    table_grad = None
    for span in spans:
        for block in range(span.start, span.stop, BLOCK):
            edges = slice(block, block + BLOCK)
            for tile in range(ROWS // 128):
                lanes = slice(tile * 128, (tile + 1) * 128)
                times = load_ref[HIST_ROW + tile : HIST_ROW + tile + 1, edges] * (1.0 / NEG)
                value = weights(score_ref[edges, lanes], times, target[edges], tile * 128)
                high_ref[edges, lanes], low_ref[edges, lanes] = halves(value)
        weight_parts = high_ref[span, :], low_ref[span, :]
        back_ref[:, span] = dot3(table_parts, weight_parts, NT)
        part = dot3((product_parts[0][:, span], product_parts[1][:, span]), weight_parts)
        table_grad = part if table_grad is None else table_grad + part
    up_re, up_im = back_ref[0:HALF, :], back_ref[HALF:DIM, :]
    lanes = slice(first, first + wide)
    multiply(up_re, up_im, s_re, s_im, True, rg_ref, lanes)
    multiply(up_re, up_im, w_re, w_im, True, sg_out, lanes)
    return table_grad, pick


def relation_grad(rg_ref, pick):
    high, low = halves(rg_ref[...])
    return dot(high, pick, NT) + dot(low, pick, NT)


def split_flat(core, grad, flat, send_out, keep_out):
    for tile in range(RELP // 128):
        flat[tile * DIM : (tile + 1) * DIM, :] = grad[:, tile * 128 : (tile + 1) * 128]
    flat[RELP // 128 * DIM : FLAT, :] = jnp.zeros((FLAT - RELP // 128 * DIM, 128), F32)
    keep_out[...] = flat[pl.ds(pl.multiple_of(core * SIDE, SIDE), SIDE), :]
    send_out[...] = flat[pl.ds(pl.multiple_of((1 - core) * SIDE, SIDE), SIDE), :]


def join_flat(core, mine_ref, other_ref, flat):
    flat[pl.ds(pl.multiple_of(core * SIDE, SIDE), SIDE), :] = mine_ref[...]
    flat[pl.ds(pl.multiple_of((1 - core) * SIDE, SIDE), SIDE), :] = other_ref[...]


def adagrad(table, state, grad):
    state = state + jnp.sum(grad * grad, axis=0, keepdims=True) * (1.0 / DIM)
    return table - grad * (RATE / jnp.sqrt(state)), state


def first_piece(
    load_ref, high_ref, low_ref, rel_high, rel_low, sg_out, rg_out, table_grad, *work
):
    table_parts, rel_parts = (high_ref[...], low_ref[...]), (rel_high[...], rel_low[...])
    table_grad[...], _ = edge_terms(load_ref, table_parts, rel_parts, work, sg_out, rg_out, 0)


def second_piece(
    core_ref,
    early_ref,
    load_ref,
    high_ref,
    low_ref,
    rel_high,
    rel_low,
    sg_ref,
    rg_ref,
    g_ref,
    sg_out,
    table_grad,
    send,
    keep,
    *work,
):
    work, rg, flat = work[:-2], work[-2], work[-1]
    table_parts, rel_parts = (high_ref[...], low_ref[...]), (rel_high[...], rel_low[...])
    first = EARLY
    sg_out[:, 0:first] = sg_ref[...]
    rg[:, 0:first] = rg_ref[...]
    grad, pick = edge_terms(load_ref, table_parts, rel_parts, work, sg_out, rg, first)
    table_grad[...] = grad + g_ref[...]
    early = one_hot(early_ref[ID_ROW : ID_ROW + 1, :].astype(jnp.int32), RELP)
    pick = jnp.concatenate([early, pick], axis=1)
    split_flat(core_ref[0], relation_grad(rg, pick), flat, send, keep)


def step_relations(core, mine_ref, other_ref, rel_ref, state_ref, flat, rel_out, state_out):
    join_flat(core, mine_ref, other_ref, flat)
    for tile in range(RELP // 128):
        lanes = slice(tile * 128, (tile + 1) * 128)
        rel_out[:, lanes], state_out[:, lanes] = adagrad(
            rel_ref[:, lanes], state_ref[:, lanes], flat[tile * DIM : (tile + 1) * DIM, :]
        )


def second_round(
    core_ref,
    mine_ref,
    other_ref,
    rel_ref,
    state_ref,
    load_ref,
    high_ref,
    low_ref,
    sg_out,
    table_grad,
    send,
    keep,
    rel_out,
    state_out,
    *work,
):
    work, rg, flat = work[:-2], work[-2], work[-1]
    core = core_ref[0]
    step_relations(core, mine_ref, other_ref, rel_ref, state_ref, flat, rel_out, state_out)
    table_grad[...], pick = edge_terms(
        load_ref, (high_ref[...], low_ref[...]), halves(rel_out[...]), work, sg_out, rg, 0
    )
    split_flat(core, relation_grad(rg, pick), flat, send, keep)


def step_entities(table_ref, state_ref, grad_ref, back_ref, edges_ref, count, which):
    pick = one_hot(live_sources(edges_ref, count, which), ROWS)
    high, low = halves(back_ref[...])
    grad = grad_ref[...] + (dot(high, pick, NT) + dot(low, pick, NT))
    return adagrad(table_ref[...], state_ref[...], grad)


def between(
    counts_ref,
    table_hbm,
    state_ref,
    grad_hbm,
    back_hbm,
    edges_hbm,
    negatives_hbm,
    table_out,
    state_out,
    high_out,
    low_out,
    load,
    table_ref,
    grad_ref,
    back_ref,
    edges_ref,
    negatives_ref,
    high_ref,
    low_ref,
    sem,
):
    copies = fetch(
        sem,
        (edges_hbm, edges_ref),
        (back_hbm, back_ref),
        (grad_hbm, grad_ref),
        (table_hbm, table_ref),
        (negatives_hbm, negatives_ref),
    )
    for copy in copies:
        copy.wait()
    table, state_out[...] = step_entities(
        table_ref, state_ref, grad_ref, back_ref, edges_ref, counts_ref[0, 0], 0
    )
    table_ref[...] = table
    parts = halves(table)
    high_ref[...], low_ref[...] = parts
    copies = fetch(sem, (table_ref, table_out), (high_ref, high_out), (low_ref, low_out))
    write_payload((load,), parts, edges_ref, negatives_ref, counts_ref[0, 1], 1)
    for copy in copies:
        copy.wait()


def last_entities(
    counts_ref,
    table_hbm,
    state_ref,
    grad_hbm,
    back_hbm,
    edges_hbm,
    table_out,
    state_out,
    table_ref,
    grad_ref,
    back_ref,
    edges_ref,
    sem,
):
    copies = fetch(
        sem,
        (edges_hbm, edges_ref),
        (back_hbm, back_ref),
        (grad_hbm, grad_ref),
        (table_hbm, table_ref),
    )
    for copy in copies:
        copy.wait()
    table, state_out[...] = step_entities(
        table_ref, state_ref, grad_ref, back_ref, edges_ref, counts_ref[0, 1], 1
    )
    table_ref[...] = table
    (copy,) = fetch(sem, (table_ref, table_out))
    copy.wait()


def last_relations(
    core_ref, mine_ref, other_ref, rel_ref, state_ref, rel_out, state_out, flat, rel, state
):
    step_relations(core_ref[0], mine_ref, other_ref, rel_ref, state_ref, flat, rel, state)
    rel_out[...] = rel[:, 0:REL]
    state_out[...] = state[:, 0:REL]


def work_shapes(wide):
    return [
        pltpu.VMEM((DIM, wide), F32),
        pltpu.VMEM((DIM, wide), F32),
        pltpu.VMEM((wide, ROWS), F32),
        pltpu.VMEM((wide, ROWS), BF16),
        pltpu.VMEM((wide, ROWS), BF16),
        pltpu.VMEM((DIM, wide), F32),
    ]


SPECS = {"s": SMEM, "v": VMEM, "h": HBM}


def call(body, ins, outs, operands, scratch=(), copies=0, grant=48 << 20):
    scratch = list(scratch) + ([pltpu.SemaphoreType.DMA((copies,))] if copies else [])
    return pl.pallas_call(
        body,
        out_shape=[out for _, out in outs],
        in_specs=[SPECS[kind] for kind in ins],
        out_specs=[SPECS[kind] for kind, _ in outs],
        scratch_shapes=scratch,
        compiler_params=params(grant),
    )(*operands)


def across(value, axis, apart):
    count = lax.axis_size(axis)
    return lax.ppermute(value, axis, [(i, i ^ apart) for i in range(count)])


def total(send, keep):
    part = (keep + across(send, C, 1)).reshape(16, SIDE // 16, 128)
    part = lax.all_to_all(part, (X, Y), 0, 0, tiled=True).sum(axis=0)
    part = jnp.broadcast_to(part[None], (8, *part.shape))
    part = lax.all_to_all(part, Z, 0, 0, tiled=True).sum(axis=0)
    part = jnp.broadcast_to(part[None], (16, *part.shape))
    part = lax.all_to_all(part, (X, Y), 0, 0, tiled=True)
    mine = part.reshape(SIDE, 128)
    return mine, across(mine, C, 1)


def body(entities, entity_state, relations, relation_state, edges, negatives, counts):
    core = lax.axis_index(C).astype(jnp.int32).reshape(1)
    table, rel, counts = entities.T, relations.T, counts.T
    edges = edges.transpose(1, 0, 2)
    state = entity_state.reshape(1, ROWS)
    late = EDGES - EARLY
    grown = shape(DIM, ROWS)
    narrow = shape(DIM, ROWS, dtype=BF16)
    wide_rel = shape(DIM, RELP, dtype=BF16)
    vmem = pltpu.VMEM
    table_mem, narrow_mem = vmem((DIM, ROWS), F32), vmem((DIM, ROWS), BF16)
    flat_mem, back_mem = vmem((FLAT, 128), F32), vmem((DIM, EDGES), F32)
    edge_mem, negative_mem = vmem((3, 2, EDGES), jnp.int32), vmem(negatives.shape, jnp.int32)
    high, low, first, second = call(
        prepare,
        "shhh",
        [("h", narrow), ("h", narrow), ("h", shape(LOAD, EARLY)), ("h", shape(LOAD, late))],
        (counts, table, edges, negatives),
        [table_mem, edge_mem, negative_mem, narrow_mem, narrow_mem]
        + [vmem((LOAD, EARLY), F32), vmem((LOAD, late), F32)],
        4,
        63 << 20,
    )
    first = across(first, Z, 4)
    second = across(second, Z, 4)
    rel, rel_state, rel_high, rel_low = call(
        pad_relations,
        "vv",
        [("v", shape(DIM, RELP)), ("v", shape(1, RELP)), ("v", wide_rel), ("v", wide_rel)],
        (rel, relation_state.reshape(1, REL)),
    )
    piece = ("v", shape(DIM, EARLY))
    back, rel_terms, grad = call(
        first_piece,
        "vvvvv",
        [piece, piece, ("v", grown)],
        (first, high, low, rel_high, rel_low),
        work_shapes(EARLY),
    )
    half = ("v", shape(SIDE, 128))
    back, grad, send, keep = call(
        second_piece,
        "svvvvvvvvv",
        [("v", shape(DIM, EDGES)), ("v", grown), half, half],
        (core, first, second, high, low, rel_high, rel_low, back, rel_terms, grad),
        work_shapes(late) + [back_mem, flat_mem],
    )
    back = across(back, Z, 4)
    mine, other = total(send, keep)
    table, state, high, low, load = call(
        between,
        "shvhhhh",
        [
            ("h", grown),
            ("v", shape(1, ROWS)),
            ("h", narrow),
            ("h", narrow),
            ("v", shape(LOAD, EDGES)),
        ],
        (counts, table, state, grad, back, edges, negatives),
        [table_mem, table_mem, back_mem, edge_mem, negative_mem, narrow_mem, narrow_mem],
        5,
        63 << 20,
    )
    load = across(load, C, 1)
    back, grad, send, keep, rel, rel_state = call(
        second_round,
        "svvvvvvv",
        [
            ("v", shape(DIM, EDGES)),
            ("v", grown),
            half,
            half,
            ("v", shape(DIM, RELP)),
            ("v", shape(1, RELP)),
        ],
        (core, mine, other, rel, rel_state, load, high, low),
        work_shapes(EDGES) + [back_mem, flat_mem],
    )
    back = across(back, C, 1)
    mine, other = total(send, keep)
    table, state = call(
        last_entities,
        "shvhhh",
        [("h", grown), ("v", shape(1, ROWS))],
        (counts, table, state, grad, back, edges),
        [table_mem, table_mem, back_mem, edge_mem],
        4,
        63 << 20,
    )
    rel, rel_state = call(
        last_relations,
        "svvvv",
        [("v", shape(DIM, REL)), ("v", shape(1, REL))],
        (core, mine, other, rel, rel_state),
        [flat_mem, vmem((DIM, RELP), F32), vmem((1, RELP), F32)],
    )
    return table.T, state.reshape(ROWS), rel.T, rel_state.reshape(REL)


def solution(mesh):
    finer = Mesh(mesh.devices.reshape(8, 4, 4, 2), DOM)
    return jax.shard_map(
        body,
        mesh=finer,
        in_specs=(
            P(DOM, None),
            P(DOM),
            P(),
            P(),
            P(None, None, DOM),
            P(None, DOM, None),
            P(None, DOM),
        ),
        out_specs=(P(DOM, None), P(DOM), P(), P()),
        check_vma=False,
    )
```

```python
import jax
import jax.numpy as jnp
from jax import lax
from jax.experimental import pallas as pl
from jax.experimental.pallas import tpu as pltpu
from jax.sharding import Mesh
from jax.sharding import PartitionSpec as P

Z, X, Y, C = "z", "x", "y", "c"
DOM = (Z, X, Y, C)
F32 = jnp.float32
BF16 = jnp.bfloat16
RATE = 0.2

ROWS = 1024
DIM = 200
HALF = DIM // 2
REL = 1345
RELP = 1536
NEG = 1000
BLOCK = 128
STEP = 256
EARLY = 256
STORE = 18
GRAD, RELATION, TABLE = 0, 1, 2
EDGES = 512
LOAD = 216
ID_ROW = 200
HIST_ROW = 208
FLAT = 2304
SIDE = FLAT // 2
TILES = 11

VMEM = pl.BlockSpec(memory_space=pltpu.VMEM)
SMEM = pl.BlockSpec(memory_space=pltpu.SMEM)
HBM = pl.BlockSpec(memory_space=pltpu.HBM)


def shape(*dims, dtype=F32):
    return jax.ShapeDtypeStruct(dims, dtype)


def params(grant):
    return pltpu.CompilerParams(vmem_limit_bytes=grant)


def halves(value):
    high = value.astype(BF16)
    return high, (value - high.astype(F32)).astype(BF16)


def dot(a, b, dims=((1,), (0,))):
    return lax.dot_general(a, b, (dims, ((), ())), preferred_element_type=F32)


NT = ((1,), (1,))


def dot3(a, b, dims=((1,), (0,))):
    return dot(a[0], b[0], dims) + (dot(a[1], b[0], dims) + dot(a[0], b[1], dims))


def one_hot(ids, count, first=0):
    places = lax.broadcasted_iota(jnp.int32, (count, ids.shape[1]), 0)
    return jnp.where(places == ids - first, 1.0, 0.0).astype(BF16)


def steps(count, size, step):
    def visit(index, carry):
        step(pl.multiple_of(index * size, size))
        return carry

    lax.fori_loop(0, count // size, visit, 0)


def histogram(ids):
    upper = lax.broadcasted_iota(jnp.int32, (8, NEG), 0)
    lower = lax.broadcasted_iota(jnp.int32, (128, NEG), 0)
    high = jnp.where(upper == (ids >> 7), 1.0, 0.0).astype(BF16)
    low = jnp.where(lower == (ids & 127), 1.0, 0.0).astype(BF16)
    return dot(high, low, NT)


def live_sources(edges_ref, count, which):
    places = lax.broadcasted_iota(jnp.int32, (1, EDGES), 1)
    return jnp.where(places < count, edges_ref[0, which : which + 1, :], -1)


def fetch(sem, *pairs):
    copies = [pltpu.make_async_copy(a, b, sem.at[i]) for i, (a, b) in enumerate(pairs)]
    for copy in copies:
        copy.start()
    return copies


def write_payload(out_refs, parts, edges_ref, negatives_ref, count, which):
    source = live_sources(edges_ref, count, which)
    pick = one_hot(source, ROWS)
    high, low = parts
    rows = dot(high, pick) + dot(low, pick)
    first = 0
    for ref in out_refs:
        wide = ref.shape[1]
        span = slice(first, first + wide)
        ref[0:DIM, :] = rows[:, span]
        ref[ID_ROW : ID_ROW + 1, :] = edges_ref[1, which : which + 1, span].astype(F32)
        ref[ID_ROW + 1 : ID_ROW + 2, :] = edges_ref[2, which : which + 1, span].astype(F32)
        ref[ID_ROW + 2 : HIST_ROW, :] = jnp.zeros((HIST_ROW - ID_ROW - 2, wide), F32)
        for block in range(wide // BLOCK):
            k = first // BLOCK + block
            ref[HIST_ROW:LOAD, block * BLOCK : (block + 1) * BLOCK] = histogram(
                negatives_ref[which, k : k + 1, :]
            )
        first += wide


def prepare(
    counts_ref,
    table_hbm,
    edges_hbm,
    negatives_hbm,
    high_out,
    low_out,
    first_out,
    second_out,
    table_ref,
    edges_ref,
    negatives_ref,
    high_ref,
    low_ref,
    first_ref,
    second_ref,
    sem,
):
    copies = fetch(
        sem, (edges_hbm, edges_ref), (table_hbm, table_ref), (negatives_hbm, negatives_ref)
    )
    for copy in copies:
        copy.wait()
    parts = halves(table_ref[...])
    high_ref[...], low_ref[...] = parts
    copies = fetch(sem, (high_ref, high_out), (low_ref, low_out))
    pieces = (first_ref, second_ref)
    write_payload(pieces, parts, edges_ref, negatives_ref, counts_ref[0, 0], 0)
    copies += fetch(sem.at[2:4], (first_ref, first_out), (second_ref, second_out))
    for copy in copies:
        copy.wait()


def pad_relations(rel_ref, state_ref, rel_out, state_out, high_out, low_out, rel, sem):
    rel[:, 10 * 128 : RELP] = jnp.zeros((DIM, RELP - 10 * 128), F32)
    rel[:, 0:REL] = rel_ref[...]
    (copy,) = fetch(sem, (rel, rel_out.at[RELATION]))
    high_out[...], low_out[...] = halves(rel[...])
    state_out[...] = jnp.ones((1, RELP), F32)
    state_out[:, 0:REL] = state_ref[...]
    copy.wait()


def multiply(a_re, a_im, b_re, b_im, conjugate, out, lanes):
    if conjugate:
        out[0:HALF, lanes] = a_re * b_re + a_im * b_im
        out[HALF:DIM, lanes] = a_im * b_re - a_re * b_im
    else:
        out[0:HALF, lanes] = a_re * b_re - a_im * b_im
        out[HALF:DIM, lanes] = a_re * b_im + a_im * b_re


def weights(scores, times, target, first_lane):
    small = jnp.exp(-jnp.abs(scores))
    large = 1.0 / (1.0 + small)
    small = small * large
    up = scores >= 0.0
    plus = jnp.where(up, large, small)
    minus = jnp.where(up, small, large)
    lanes = lax.broadcasted_iota(jnp.int32, (1, 128), 1) + first_lane
    return plus * times - jnp.where(lanes == target, minus, 0.0)


def edge_terms(load_ref, high_ref, low_ref, rel_parts, work, grad_ref, sg_out, rg_ref, first, put):
    w_ref, q_ref, qh_ref, ql_ref, score_ref, wh_ref, wl_ref, back_ref, target_ref = work
    wide = load_ref.shape[1]
    ids = load_ref[ID_ROW : ID_ROW + 1, :].astype(jnp.int32)
    w_ref[...] = jnp.zeros((DIM, wide), F32)

    def gather(start):
        pick = one_hot(ids, STEP, start)
        high, low = rel_parts(start)
        w_ref[...] += dot(high, pick) + dot(low, pick)

    steps(RELP, STEP, gather)
    s_re, s_im = load_ref[0:HALF, :], load_ref[HALF:DIM, :]
    w_re, w_im = w_ref[0:HALF, :], w_ref[HALF:DIM, :]
    multiply(s_re, s_im, w_re, w_im, False, q_ref, slice(None))
    product = q_ref[...]
    qh_ref[...], ql_ref[...] = halves(product)
    target = load_ref[ID_ROW : ID_ROW + 8, :].T[:, 1:2].astype(jnp.int32)
    target_ref[...] = jnp.broadcast_to(target, (wide, BLOCK))
    turned = halves(product.T)

    def score(start):
        lanes = pl.ds(start, STEP)
        score_ref[:, lanes] = dot3(turned, (high_ref[:, lanes], low_ref[:, lanes]))

    steps(ROWS, STEP, score)

    def weigh(start):
        edges = pl.ds(start, BLOCK)
        for tile in range(ROWS // BLOCK):
            lanes = slice(tile * BLOCK, (tile + 1) * BLOCK)
            times = load_ref[HIST_ROW + tile : HIST_ROW + tile + 1, edges] * (1.0 / NEG)
            value = weights(score_ref[edges, lanes], times, target_ref[edges, :], tile * BLOCK)
            wh_ref[edges, lanes], wl_ref[edges, lanes] = halves(value)

    steps(wide, BLOCK, weigh)

    def backward(start):
        edges = pl.ds(start, STEP)
        parts = wh_ref[edges, :], wl_ref[edges, :]
        back_ref[:, edges] = dot3((high_ref[...], low_ref[...]), parts, NT)

    steps(wide, STEP, backward)

    def table(start):
        lanes = pl.ds(start, STEP)
        parts = wh_ref[:, lanes], wl_ref[:, lanes]
        grad_ref[:, lanes] = dot3((qh_ref[...], ql_ref[...]), parts)

    steps(ROWS, STEP, table)
    copies = put()
    up_re, up_im = back_ref[0:HALF, :], back_ref[HALF:DIM, :]
    lanes = slice(first, first + wide)
    multiply(up_re, up_im, s_re, s_im, True, rg_ref, lanes)
    multiply(up_re, up_im, w_re, w_im, True, sg_out, lanes)
    return copies


def relation_grad(core, rg_ref, ids, flat, send_out, keep_out):
    high, low = halves(rg_ref[...])

    def scatter(start):
        pick = one_hot(ids, STEP, start)
        grad = dot(high, pick, NT) + dot(low, pick, NT)
        row = pl.multiple_of(start // BLOCK * DIM, 8)
        flat[pl.ds(row, DIM), :] = grad[:, 0:BLOCK]
        flat[pl.ds(row + DIM, DIM), :] = grad[:, BLOCK:STEP]

    steps(RELP, STEP, scatter)
    keep_out[...] = flat[pl.ds(pl.multiple_of(core * SIDE, SIDE), SIDE), :]
    send_out[...] = flat[pl.ds(pl.multiple_of((1 - core) * SIDE, SIDE), SIDE), :]


def join_flat(core, mine_ref, other_ref, flat):
    flat[pl.ds(pl.multiple_of(core * SIDE, SIDE), SIDE), :] = mine_ref[...]
    flat[pl.ds(pl.multiple_of((1 - core) * SIDE, SIDE), SIDE), :] = other_ref[...]


def adagrad(table, state, grad):
    state = state + jnp.sum(grad * grad, axis=0, keepdims=True) * (1.0 / DIM)
    return table - grad * (RATE / jnp.sqrt(state)), state


def parts_of(high_ref, low_ref):
    def parts(start):
        return high_ref[:, pl.ds(start, STEP)], low_ref[:, pl.ds(start, STEP)]

    return parts


def entities_of(store, plane):
    return store.at[plane, :, 0:ROWS]


def first_piece(
    load_ref, high_ref, low_ref, rel_high, rel_low, _, sg_out, rg_out, store, *work
):
    work, grad_ref, sem = work[:-2], work[-2], work[-1]

    def put():
        return fetch(sem, (grad_ref, entities_of(store, GRAD)))

    parts = parts_of(rel_high, rel_low)
    copies = edge_terms(load_ref, high_ref, low_ref, parts, work, grad_ref, sg_out, rg_out, 0, put)
    for copy in copies:
        copy.wait()


def second_piece(
    core_ref,
    early_ref,
    load_ref,
    high_ref,
    low_ref,
    rel_high,
    rel_low,
    sg_ref,
    rg_ref,
    _,
    sg_out,
    send,
    keep,
    store,
    *work,
):
    work, rg, flat, grad_ref, g_ref, sem = work[:-5], *work[-5:]
    (g_copy,) = fetch(sem, (entities_of(store, GRAD), g_ref))

    def put():
        g_copy.wait()
        grad_ref[...] += g_ref[...]
        return fetch(sem, (grad_ref, entities_of(store, GRAD)))

    parts = parts_of(rel_high, rel_low)
    sg_out[:, 0:EARLY] = sg_ref[...]
    rg[:, 0:EARLY] = rg_ref[...]
    copies = edge_terms(
        load_ref, high_ref, low_ref, parts, work, grad_ref, sg_out, rg, EARLY, put
    )
    row = slice(ID_ROW, ID_ROW + 1)
    ids = jnp.concatenate([early_ref[row, :], load_ref[row, :]], axis=1).astype(jnp.int32)
    relation_grad(core_ref[0], rg, ids, flat, send, keep)
    for copy in copies:
        copy.wait()


def step_relations(core, mine_ref, other_ref, rel_ref, state_ref, flat, rel_out, state_out):
    join_flat(core, mine_ref, other_ref, flat)

    def step(start):
        lanes = pl.ds(start, BLOCK)
        row = pl.multiple_of(start // BLOCK * DIM, 8)
        rel_out[:, lanes], state_out[:, lanes] = adagrad(
            rel_ref[:, lanes], state_ref[:, lanes], flat[pl.ds(row, DIM), :]
        )

    steps(TILES * BLOCK, BLOCK, step)
    rest = slice(TILES * BLOCK, RELP)
    rel_out[:, rest] = jnp.zeros((DIM, RELP - TILES * BLOCK), F32)
    state_out[:, rest] = state_ref[:, rest]


def second_round(
    core_ref,
    mine_ref,
    other_ref,
    state_ref,
    load_ref,
    _,
    sg_out,
    send,
    keep,
    state_out,
    store,
    *work,
):
    work, rg, flat, old_ref, rel_ref, high_ref, low_ref, grad_ref, sem = work[:-8], *work[-8:]
    rel_copy, table_copy = fetch(
        sem, (store.at[RELATION], old_ref), (entities_of(store, TABLE), grad_ref)
    )
    core = core_ref[0]
    rel_copy.wait()
    step_relations(core, mine_ref, other_ref, old_ref, state_ref, flat, rel_ref, state_out)
    (rel_copy,) = fetch(sem, (rel_ref, store.at[RELATION]))
    table_copy.wait()
    high_ref[...], low_ref[...] = halves(grad_ref[...])

    def parts(start):
        return halves(rel_ref[:, pl.ds(start, STEP)])

    def put():
        return fetch(sem.at[1:2], (grad_ref, entities_of(store, GRAD)))

    copies = edge_terms(load_ref, high_ref, low_ref, parts, work, grad_ref, sg_out, rg, 0, put)
    ids = load_ref[ID_ROW : ID_ROW + 1, :].astype(jnp.int32)
    relation_grad(core, rg, ids, flat, send, keep)
    for copy in [rel_copy, *copies]:
        copy.wait()


def step_entities(table_ref, state_ref, grad_ref, back_ref, edges_ref, count, which):
    pick = one_hot(live_sources(edges_ref, count, which), ROWS)
    high, low = halves(back_ref[...])
    grad = grad_ref[...] + (dot(high, pick, NT) + dot(low, pick, NT))
    return adagrad(table_ref[...], state_ref[...], grad)


def between(
    counts_ref,
    table_hbm,
    state_ref,
    _,
    back_hbm,
    edges_hbm,
    negatives_hbm,
    state_out,
    store,
    load,
    table_ref,
    grad_ref,
    back_ref,
    edges_ref,
    negatives_ref,
    sem,
):
    copies = fetch(
        sem,
        (edges_hbm, edges_ref),
        (back_hbm, back_ref),
        (entities_of(store, GRAD), grad_ref),
        (table_hbm, table_ref),
        (negatives_hbm, negatives_ref),
    )
    for copy in copies:
        copy.wait()
    table, state_out[...] = step_entities(
        table_ref, state_ref, grad_ref, back_ref, edges_ref, counts_ref[0, 0], 0
    )
    table_ref[...] = table
    (copy,) = fetch(sem, (table_ref, entities_of(store, TABLE)))
    write_payload((load,), halves(table), edges_ref, negatives_ref, counts_ref[0, 1], 1)
    copy.wait()


def last_entities(
    counts_ref,
    state_ref,
    store,
    back_hbm,
    edges_hbm,
    table_out,
    state_out,
    table_ref,
    grad_ref,
    back_ref,
    edges_ref,
    sem,
):
    copies = fetch(
        sem,
        (edges_hbm, edges_ref),
        (back_hbm, back_ref),
        (entities_of(store, GRAD), grad_ref),
        (entities_of(store, TABLE), table_ref),
    )
    for copy in copies:
        copy.wait()
    table, state_out[...] = step_entities(
        table_ref, state_ref, grad_ref, back_ref, edges_ref, counts_ref[0, 1], 1
    )
    table_ref[...] = table
    (copy,) = fetch(sem, (table_ref, table_out))
    copy.wait()


def last_relations(
    core_ref,
    mine_ref,
    other_ref,
    store,
    state_ref,
    rel_out,
    state_out,
    flat,
    old_ref,
    rel,
    state,
    sem,
):
    (copy,) = fetch(sem, (store.at[RELATION], old_ref))
    copy.wait()
    step_relations(core_ref[0], mine_ref, other_ref, old_ref, state_ref, flat, rel, state)
    rel_out[...] = rel[:, 0:REL]
    state_out[...] = state[:, 0:REL]


def work_shapes(wide):
    return [
        pltpu.VMEM((DIM, wide), F32),
        pltpu.VMEM((DIM, wide), F32),
        pltpu.VMEM((DIM, wide), BF16),
        pltpu.VMEM((DIM, wide), BF16),
        pltpu.VMEM((wide, ROWS), F32),
        pltpu.VMEM((wide, ROWS), BF16),
        pltpu.VMEM((wide, ROWS), BF16),
        pltpu.VMEM((DIM, wide), F32),
        pltpu.VMEM((wide, BLOCK), jnp.int32),
    ]


SPECS = {"s": SMEM, "v": VMEM, "h": HBM}


def call(body, ins, outs, operands, scratch=(), copies=0, grant=48 << 20, alias=None):
    scratch = list(scratch) + ([pltpu.SemaphoreType.DMA((copies,))] if copies else [])
    return pl.pallas_call(
        body,
        out_shape=[out for _, out in outs],
        in_specs=[SPECS[kind] for kind in ins],
        out_specs=[SPECS[kind] for kind, _ in outs],
        scratch_shapes=scratch,
        input_output_aliases=alias or {},
        compiler_params=params(grant),
    )(*operands)


def across(value, axis, apart):
    count = lax.axis_size(axis)
    return lax.ppermute(value, axis, [(i, i ^ apart) for i in range(count)])


def total(send, keep):
    part = (keep + across(send, C, 1)).reshape(16, SIDE // 16, 128)
    part = lax.all_to_all(part, (X, Y), 0, 0, tiled=True).sum(axis=0)
    part = jnp.broadcast_to(part[None], (8, *part.shape))
    part = lax.all_to_all(part, Z, 0, 0, tiled=True).sum(axis=0)
    part = jnp.broadcast_to(part[None], (16, *part.shape))
    part = lax.all_to_all(part, (X, Y), 0, 0, tiled=True)
    mine = part.reshape(SIDE, 128)
    return mine, across(mine, C, 1)


def body(entities, entity_state, relations, relation_state, edges, negatives, counts):
    core = lax.axis_index(C).astype(jnp.int32).reshape(1)
    table, rel, counts = entities.T, relations.T, counts.T
    edges = edges.transpose(1, 0, 2)
    state = entity_state.reshape(1, ROWS)
    late = EDGES - EARLY
    grown = shape(DIM, ROWS)
    narrow = shape(DIM, ROWS, dtype=BF16)
    wide_rel = shape(DIM, RELP, dtype=BF16)
    vmem = pltpu.VMEM
    table_mem, narrow_mem = vmem((DIM, ROWS), F32), vmem((DIM, ROWS), BF16)
    flat_mem = vmem((RELP // BLOCK * DIM, 128), F32)
    back_mem, rel_mem = vmem((DIM, EDGES), F32), vmem((DIM, RELP), F32)
    edge_mem, negative_mem = vmem((3, 2, EDGES), jnp.int32), vmem(negatives.shape, jnp.int32)
    high, low, first, second = call(
        prepare,
        "shhh",
        [("h", narrow), ("h", narrow), ("h", shape(LOAD, EARLY)), ("h", shape(LOAD, late))],
        (counts, table, edges, negatives),
        [table_mem, edge_mem, negative_mem, narrow_mem, narrow_mem]
        + [vmem((LOAD, EARLY), F32), vmem((LOAD, late), F32)],
        4,
        63 << 20,
    )
    first = across(first, Z, 4)
    second = across(second, Z, 4)
    store_out = ("h", shape(STORE, DIM, RELP))
    store, rel_state, rel_high, rel_low = call(
        pad_relations,
        "vv",
        [store_out, ("v", shape(1, RELP)), ("v", wide_rel), ("v", wide_rel)],
        (rel, relation_state.reshape(1, REL)),
        [rel_mem],
        1,
    )
    piece = ("v", shape(DIM, EARLY))
    back, rel_terms, store = call(
        first_piece,
        "vvvvvh",
        [piece, piece, store_out],
        (first, high, low, rel_high, rel_low, store),
        work_shapes(EARLY) + [table_mem],
        1,
        alias={5: 2},
    )
    half = ("v", shape(SIDE, 128))
    back, send, keep, store = call(
        second_piece,
        "svvvvvvvvh",
        [("v", shape(DIM, EDGES)), half, half, store_out],
        (core, first, second, high, low, rel_high, rel_low, back, rel_terms, store),
        work_shapes(late) + [back_mem, flat_mem, table_mem, table_mem],
        1,
        alias={9: 3},
    )
    back = across(back, Z, 4)
    mine, other = total(send, keep)
    state, store, load = call(
        between,
        "shvhhhh",
        [("v", shape(1, ROWS)), store_out, ("v", shape(LOAD, EDGES))],
        (counts, table, state, store, back, edges, negatives),
        [table_mem, table_mem, back_mem, edge_mem, negative_mem],
        5,
        63 << 20,
        {3: 1},
    )
    load = across(load, C, 1)
    back, send, keep, rel_state, store = call(
        second_round,
        "svvvvh",
        [("v", shape(DIM, EDGES)), half, half, ("v", shape(1, RELP)), store_out],
        (core, mine, other, rel_state, load, store),
        work_shapes(EDGES)
        + [back_mem, flat_mem, rel_mem, rel_mem, narrow_mem, narrow_mem, table_mem],
        2,
        alias={5: 4},
    )
    back = across(back, C, 1)
    mine, other = total(send, keep)
    table, state = call(
        last_entities,
        "svhhh",
        [("h", grown), ("v", shape(1, ROWS))],
        (counts, state, store, back, edges),
        [table_mem, table_mem, back_mem, edge_mem],
        4,
        63 << 20,
    )
    rel, rel_state = call(
        last_relations,
        "svvhv",
        [("v", shape(DIM, REL)), ("v", shape(1, REL))],
        (core, mine, other, store, rel_state),
        [flat_mem, rel_mem, rel_mem, vmem((1, RELP), F32)],
        1,
    )
    return table.T, state.reshape(ROWS), rel.T, rel_state.reshape(REL)


def solution(mesh):
    finer = Mesh(mesh.devices.reshape(8, 4, 4, 2), DOM)
    return jax.shard_map(
        body,
        mesh=finer,
        in_specs=(
            P(DOM, None),
            P(DOM),
            P(),
            P(),
            P(None, None, DOM),
            P(None, DOM, None),
            P(None, DOM),
        ),
        out_specs=(P(DOM, None), P(DOM), P(), P()),
        check_vma=False,
    )
```

```python
import jax
import jax.numpy as jnp
from jax import lax
from jax.experimental import pallas as pl
from jax.experimental.pallas import tpu as pltpu
from jax.sharding import Mesh
from jax.sharding import PartitionSpec as P

Z, X, Y, C = "z", "x", "y", "c"
DOM = (Z, X, Y, C)
F32 = jnp.float32
BF16 = jnp.bfloat16
RATE = 0.2

ROWS = 1024
DIM = 200
HALF = DIM // 2
REL = 1345
RELP = 1408
NEG = 1000
BLOCK = 128
STEP = 256
EARLY = 256
STORE = 18
GRAD, RELATION, TABLE = 0, 1, 2
EDGES = 512
LOAD = 216
ID_ROW = 200
HIST_ROW = 208
FLAT = 2304
SIDE = FLAT // 2

VMEM = pl.BlockSpec(memory_space=pltpu.VMEM)
SMEM = pl.BlockSpec(memory_space=pltpu.SMEM)
HBM = pl.BlockSpec(memory_space=pltpu.HBM)


def shape(*dims, dtype=F32):
    return jax.ShapeDtypeStruct(dims, dtype)


def params(grant):
    return pltpu.CompilerParams(vmem_limit_bytes=grant)


def halves(value):
    high = value.astype(BF16)
    return high, (value - high.astype(F32)).astype(BF16)


def dot(a, b, dims=((1,), (0,))):
    return lax.dot_general(a, b, (dims, ((), ())), preferred_element_type=F32)


NT = ((1,), (1,))


def dot3(a, b, dims=((1,), (0,))):
    return dot(a[0], b[0], dims) + (dot(a[1], b[0], dims) + dot(a[0], b[1], dims))


def one_hot(ids, count):
    places = lax.broadcasted_iota(jnp.int32, (count, ids.shape[1]), 0)
    return jnp.where(places == ids, 1.0, 0.0).astype(BF16)


def histogram(ids):
    upper = lax.broadcasted_iota(jnp.int32, (8, NEG), 0)
    lower = lax.broadcasted_iota(jnp.int32, (128, NEG), 0)
    high = jnp.where(upper == (ids >> 7), 1.0, 0.0).astype(BF16)
    low = jnp.where(lower == (ids & 127), 1.0, 0.0).astype(BF16)
    return dot(high, low, NT)


def live_sources(edges_ref, count, which):
    places = lax.broadcasted_iota(jnp.int32, (1, EDGES), 1)
    return jnp.where(places < count, edges_ref[0, which : which + 1, :], -1)


def fetch(sem, *pairs):
    copies = [pltpu.make_async_copy(a, b, sem.at[i]) for i, (a, b) in enumerate(pairs)]
    for copy in copies:
        copy.start()
    return copies


def write_payload(out_refs, parts, edges_ref, negatives_ref, count, which):
    source = live_sources(edges_ref, count, which)
    pick = one_hot(source, ROWS)
    high, low = parts
    rows = dot(high, pick) + dot(low, pick)
    first = 0
    for ref in out_refs:
        wide = ref.shape[1]
        span = slice(first, first + wide)
        ref[0:DIM, :] = rows[:, span]
        ref[ID_ROW : ID_ROW + 1, :] = edges_ref[1, which : which + 1, span].astype(F32)
        ref[ID_ROW + 1 : ID_ROW + 2, :] = edges_ref[2, which : which + 1, span].astype(F32)
        ref[ID_ROW + 2 : HIST_ROW, :] = jnp.zeros((HIST_ROW - ID_ROW - 2, wide), F32)
        for block in range(wide // BLOCK):
            k = first // BLOCK + block
            ref[HIST_ROW:LOAD, block * BLOCK : (block + 1) * BLOCK] = histogram(
                negatives_ref[which, k : k + 1, :]
            )
        first += wide


def prepare(
    counts_ref,
    table_hbm,
    edges_hbm,
    negatives_hbm,
    first_out,
    second_out,
    table_ref,
    edges_ref,
    negatives_ref,
    first_ref,
    second_ref,
    sem,
):
    copies = fetch(
        sem, (edges_hbm, edges_ref), (table_hbm, table_ref), (negatives_hbm, negatives_ref)
    )
    for copy in copies:
        copy.wait()
    pieces = (first_ref, second_ref)
    parts = halves(table_ref[...])
    write_payload(pieces, parts, edges_ref, negatives_ref, counts_ref[0, 0], 0)
    for copy in fetch(sem, (first_ref, first_out), (second_ref, second_out)):
        copy.wait()


def settle(
    table_ref,
    rel_ref,
    state_ref,
    store,
    state_out,
    rel_high,
    rel_low,
    table_high,
    table_low,
    rel,
    sem,
):
    rel[:, 10 * 128 : RELP] = jnp.zeros((DIM, RELP - 10 * 128), F32)
    rel[:, 0:REL] = rel_ref[...]
    (copy,) = fetch(sem, (rel, store.at[RELATION]))
    rel_high[...], rel_low[...] = halves(rel[...])
    table_high[...], table_low[...] = halves(table_ref[...])
    state_out[...] = jnp.ones((1, RELP), F32)
    state_out[:, 0:REL] = state_ref[...]
    copy.wait()


def multiply(a_re, a_im, b_re, b_im, conjugate, out, lanes):
    if conjugate:
        out[0:HALF, lanes] = a_re * b_re + a_im * b_im
        out[HALF:DIM, lanes] = a_im * b_re - a_re * b_im
    else:
        out[0:HALF, lanes] = a_re * b_re - a_im * b_im
        out[HALF:DIM, lanes] = a_re * b_im + a_im * b_re


def weights(scores, times, target, first_lane):
    small = jnp.exp(-jnp.abs(scores))
    large = 1.0 / (1.0 + small)
    small = small * large
    up = scores >= 0.0
    plus = jnp.where(up, large, small)
    minus = jnp.where(up, small, large)
    lanes = lax.broadcasted_iota(jnp.int32, (1, 128), 1) + first_lane
    return plus * times - jnp.where(lanes == target, minus, 0.0)


def edge_terms(load_ref, table_parts, rel_parts, work, sg_out, rg_ref, first, put):
    w_ref, q_ref, score_ref, high_ref, low_ref, back_ref = work
    wide = load_ref.shape[1]
    pick = one_hot(load_ref[ID_ROW : ID_ROW + 1, :].astype(jnp.int32), RELP)
    w_ref[...] = dot(rel_parts[0], pick) + dot(rel_parts[1], pick)
    s_re, s_im = load_ref[0:HALF, :], load_ref[HALF:DIM, :]
    w_re, w_im = w_ref[0:HALF, :], w_ref[HALF:DIM, :]
    multiply(s_re, s_im, w_re, w_im, False, q_ref, slice(None))
    product = q_ref[...]
    product_parts = halves(product)
    target = load_ref[ID_ROW : ID_ROW + 8, :].T[:, 1:2].astype(jnp.int32)
    turned = halves(product.T)
    spans = [slice(start, min(start + STEP, wide)) for start in range(0, wide, STEP)]
    for edges in spans:
        score_ref[edges, :] = dot3((turned[0][edges], turned[1][edges]), table_parts)
    table_grad = None
    for span in spans:
        for block in range(span.start, span.stop, BLOCK):
            edges = slice(block, block + BLOCK)
            for tile in range(ROWS // 128):
                lanes = slice(tile * 128, (tile + 1) * 128)
                times = load_ref[HIST_ROW + tile : HIST_ROW + tile + 1, edges] * (1.0 / NEG)
                value = weights(score_ref[edges, lanes], times, target[edges], tile * 128)
                high_ref[edges, lanes], low_ref[edges, lanes] = halves(value)
        weight_parts = high_ref[span, :], low_ref[span, :]
        back_ref[:, span] = dot3(table_parts, weight_parts, NT)
        part = dot3((product_parts[0][:, span], product_parts[1][:, span]), weight_parts)
        table_grad = part if table_grad is None else table_grad + part
    copies = put(table_grad)
    up_re, up_im = back_ref[0:HALF, :], back_ref[HALF:DIM, :]
    lanes = slice(first, first + wide)
    multiply(up_re, up_im, s_re, s_im, True, rg_ref, lanes)
    multiply(up_re, up_im, w_re, w_im, True, sg_out, lanes)
    return pick, copies


def relation_grad(rg_ref, pick):
    high, low = halves(rg_ref[...])
    return dot(high, pick, NT) + dot(low, pick, NT)


def split_flat(core, grad, flat, send_out, keep_out):
    for tile in range(RELP // 128):
        flat[tile * DIM : (tile + 1) * DIM, :] = grad[:, tile * 128 : (tile + 1) * 128]
    flat[RELP // 128 * DIM : FLAT, :] = jnp.zeros((FLAT - RELP // 128 * DIM, 128), F32)
    keep_out[...] = flat[pl.ds(pl.multiple_of(core * SIDE, SIDE), SIDE), :]
    send_out[...] = flat[pl.ds(pl.multiple_of((1 - core) * SIDE, SIDE), SIDE), :]


def join_flat(core, mine_ref, other_ref, flat):
    flat[pl.ds(pl.multiple_of(core * SIDE, SIDE), SIDE), :] = mine_ref[...]
    flat[pl.ds(pl.multiple_of((1 - core) * SIDE, SIDE), SIDE), :] = other_ref[...]


def adagrad(table, state, grad):
    state = state + jnp.sum(grad * grad, axis=0, keepdims=True) * (1.0 / DIM)
    return table - grad * (RATE / jnp.sqrt(state)), state


def entities_of(store, plane):
    return store.at[plane, :, 0:ROWS]


def first_piece(
    load_ref, high_ref, low_ref, rel_high, rel_low, _, sg_out, rg_out, store, *work
):
    work, grad_ref, sem = work[:-2], work[-2], work[-1]

    def put(value):
        grad_ref[...] = value
        return fetch(sem, (grad_ref, entities_of(store, GRAD)))

    table_parts, rel_parts = (high_ref[...], low_ref[...]), (rel_high[...], rel_low[...])
    _, copies = edge_terms(load_ref, table_parts, rel_parts, work, sg_out, rg_out, 0, put)
    for copy in copies:
        copy.wait()


def second_piece(
    core_ref,
    early_ref,
    load_ref,
    high_ref,
    low_ref,
    rel_high,
    rel_low,
    sg_ref,
    rg_ref,
    _,
    sg_out,
    send,
    keep,
    store,
    *work,
):
    work, rg, flat, grad_ref, g_ref, sem = work[:-5], *work[-5:]
    (g_copy,) = fetch(sem, (entities_of(store, GRAD), g_ref))

    def put(value):
        g_copy.wait()
        grad_ref[...] = value + g_ref[...]
        return fetch(sem, (grad_ref, entities_of(store, GRAD)))

    table_parts, rel_parts = (high_ref[...], low_ref[...]), (rel_high[...], rel_low[...])
    sg_out[:, 0:EARLY] = sg_ref[...]
    rg[:, 0:EARLY] = rg_ref[...]
    pick, copies = edge_terms(load_ref, table_parts, rel_parts, work, sg_out, rg, EARLY, put)
    early = one_hot(early_ref[ID_ROW : ID_ROW + 1, :].astype(jnp.int32), RELP)
    pick = jnp.concatenate([early, pick], axis=1)
    split_flat(core_ref[0], relation_grad(rg, pick), flat, send, keep)
    for copy in copies:
        copy.wait()


def step_relations(core, mine_ref, other_ref, rel_ref, state_ref, flat, rel_out, state_out):
    join_flat(core, mine_ref, other_ref, flat)
    for tile in range(RELP // 128):
        lanes = slice(tile * 128, (tile + 1) * 128)
        rel_out[:, lanes], state_out[:, lanes] = adagrad(
            rel_ref[:, lanes], state_ref[:, lanes], flat[tile * DIM : (tile + 1) * DIM, :]
        )


def second_round(
    core_ref,
    mine_ref,
    other_ref,
    state_ref,
    load_ref,
    _,
    sg_out,
    send,
    keep,
    state_out,
    store,
    *work,
):
    work, rg, flat, old_ref, rel_ref, grad_ref, sem = work[:-6], *work[-6:]
    rel_copy, table_copy = fetch(
        sem, (store.at[RELATION], old_ref), (entities_of(store, TABLE), grad_ref)
    )
    core = core_ref[0]
    rel_copy.wait()
    step_relations(core, mine_ref, other_ref, old_ref, state_ref, flat, rel_ref, state_out)
    (rel_copy,) = fetch(sem, (rel_ref, store.at[RELATION]))
    table_copy.wait()
    table_parts = halves(grad_ref[...])

    def put(value):
        grad_ref[...] = value
        return fetch(sem.at[1:2], (grad_ref, entities_of(store, GRAD)))

    rel_parts = halves(rel_ref[...])
    pick, copies = edge_terms(load_ref, table_parts, rel_parts, work, sg_out, rg, 0, put)
    split_flat(core, relation_grad(rg, pick), flat, send, keep)
    for copy in [rel_copy, *copies]:
        copy.wait()


def step_entities(table_ref, state_ref, grad_ref, back_ref, edges_ref, count, which):
    pick = one_hot(live_sources(edges_ref, count, which), ROWS)
    high, low = halves(back_ref[...])
    grad = grad_ref[...] + (dot(high, pick, NT) + dot(low, pick, NT))
    return adagrad(table_ref[...], state_ref[...], grad)


def between(
    counts_ref,
    table_hbm,
    state_ref,
    _,
    back_hbm,
    edges_hbm,
    negatives_hbm,
    state_out,
    store,
    load,
    table_ref,
    grad_ref,
    back_ref,
    edges_ref,
    negatives_ref,
    sem,
):
    copies = fetch(
        sem,
        (edges_hbm, edges_ref),
        (back_hbm, back_ref),
        (entities_of(store, GRAD), grad_ref),
        (table_hbm, table_ref),
        (negatives_hbm, negatives_ref),
    )
    for copy in copies:
        copy.wait()
    table, state_out[...] = step_entities(
        table_ref, state_ref, grad_ref, back_ref, edges_ref, counts_ref[0, 0], 0
    )
    table_ref[...] = table
    (copy,) = fetch(sem, (table_ref, entities_of(store, TABLE)))
    write_payload((load,), halves(table), edges_ref, negatives_ref, counts_ref[0, 1], 1)
    copy.wait()


def last_entities(
    counts_ref,
    state_ref,
    store,
    back_hbm,
    edges_hbm,
    table_out,
    state_out,
    table_ref,
    grad_ref,
    back_ref,
    edges_ref,
    sem,
):
    copies = fetch(
        sem,
        (edges_hbm, edges_ref),
        (back_hbm, back_ref),
        (entities_of(store, GRAD), grad_ref),
        (entities_of(store, TABLE), table_ref),
    )
    for copy in copies:
        copy.wait()
    table, state_out[...] = step_entities(
        table_ref, state_ref, grad_ref, back_ref, edges_ref, counts_ref[0, 1], 1
    )
    table_ref[...] = table
    (copy,) = fetch(sem, (table_ref, table_out))
    copy.wait()


def last_relations(
    core_ref,
    mine_ref,
    other_ref,
    store,
    state_ref,
    rel_out,
    state_out,
    flat,
    old_ref,
    rel,
    state,
    sem,
):
    (copy,) = fetch(sem, (store.at[RELATION], old_ref))
    copy.wait()
    step_relations(core_ref[0], mine_ref, other_ref, old_ref, state_ref, flat, rel, state)
    rel_out[...] = rel[:, 0:REL]
    state_out[...] = state[:, 0:REL]


def work_shapes(wide):
    return [
        pltpu.VMEM((DIM, wide), F32),
        pltpu.VMEM((DIM, wide), F32),
        pltpu.VMEM((wide, ROWS), F32),
        pltpu.VMEM((wide, ROWS), BF16),
        pltpu.VMEM((wide, ROWS), BF16),
        pltpu.VMEM((DIM, wide), F32),
    ]


SPECS = {"s": SMEM, "v": VMEM, "h": HBM}


def call(body, ins, outs, operands, scratch=(), copies=0, grant=48 << 20, alias=None):
    scratch = list(scratch) + ([pltpu.SemaphoreType.DMA((copies,))] if copies else [])
    return pl.pallas_call(
        body,
        out_shape=[out for _, out in outs],
        in_specs=[SPECS[kind] for kind in ins],
        out_specs=[SPECS[kind] for kind, _ in outs],
        scratch_shapes=scratch,
        input_output_aliases=alias or {},
        compiler_params=params(grant),
    )(*operands)


def across(value, axis, apart):
    count = lax.axis_size(axis)
    return lax.ppermute(value, axis, [(i, i ^ apart) for i in range(count)])


def total(send, keep):
    part = (keep + across(send, C, 1)).reshape(16, SIDE // 16, 128)
    part = lax.all_to_all(part, (X, Y), 0, 0, tiled=True).sum(axis=0)
    part = jnp.broadcast_to(part[None], (8, *part.shape))
    part = lax.all_to_all(part, Z, 0, 0, tiled=True).sum(axis=0)
    part = jnp.broadcast_to(part[None], (16, *part.shape))
    part = lax.all_to_all(part, (X, Y), 0, 0, tiled=True)
    mine = part.reshape(SIDE, 128)
    return mine, across(mine, C, 1)


def body(entities, entity_state, relations, relation_state, edges, negatives, counts):
    core = lax.axis_index(C).astype(jnp.int32).reshape(1)
    table, rel, counts = entities.T, relations.T, counts.T
    edges = edges.transpose(1, 0, 2)
    state = entity_state.reshape(1, ROWS)
    late = EDGES - EARLY
    grown = shape(DIM, ROWS)
    narrow = shape(DIM, ROWS, dtype=BF16)
    wide_rel = shape(DIM, RELP, dtype=BF16)
    vmem = pltpu.VMEM
    table_mem = vmem((DIM, ROWS), F32)
    flat_mem = vmem((FLAT, 128), F32)
    back_mem, rel_mem = vmem((DIM, EDGES), F32), vmem((DIM, RELP), F32)
    edge_mem, negative_mem = vmem((3, 2, EDGES), jnp.int32), vmem(negatives.shape, jnp.int32)
    first, second = call(
        prepare,
        "shhh",
        [("h", shape(LOAD, EARLY)), ("h", shape(LOAD, late))],
        (counts, table, edges, negatives),
        [table_mem, edge_mem, negative_mem, vmem((LOAD, EARLY), F32), vmem((LOAD, late), F32)],
        3,
        63 << 20,
    )
    first = across(first, Z, 4)
    second = across(second, Z, 4)
    store_out = ("h", shape(STORE, DIM, RELP))
    store, rel_state, rel_high, rel_low, high, low = call(
        settle,
        "vvv",
        [store_out, ("v", shape(1, RELP))] + [("v", wide_rel)] * 2 + [("v", narrow)] * 2,
        (table, rel, relation_state.reshape(1, REL)),
        [rel_mem],
        1,
    )
    piece = ("v", shape(DIM, EARLY))
    back, rel_terms, store = call(
        first_piece,
        "vvvvvh",
        [piece, piece, store_out],
        (first, high, low, rel_high, rel_low, store),
        work_shapes(EARLY) + [table_mem],
        1,
        alias={5: 2},
    )
    half = ("v", shape(SIDE, 128))
    back, send, keep, store = call(
        second_piece,
        "svvvvvvvvh",
        [("v", shape(DIM, EDGES)), half, half, store_out],
        (core, first, second, high, low, rel_high, rel_low, back, rel_terms, store),
        work_shapes(late) + [back_mem, flat_mem, table_mem, table_mem],
        1,
        alias={9: 3},
    )
    back = across(back, Z, 4)
    mine, other = total(send, keep)
    state, store, load = call(
        between,
        "shvhhhh",
        [("v", shape(1, ROWS)), store_out, ("v", shape(LOAD, EDGES))],
        (counts, table, state, store, back, edges, negatives),
        [table_mem, table_mem, back_mem, edge_mem, negative_mem],
        5,
        63 << 20,
        {3: 1},
    )
    load = across(load, C, 1)
    back, send, keep, rel_state, store = call(
        second_round,
        "svvvvh",
        [("v", shape(DIM, EDGES)), half, half, ("v", shape(1, RELP)), store_out],
        (core, mine, other, rel_state, load, store),
        work_shapes(EDGES)
        + [back_mem, flat_mem, rel_mem, rel_mem, table_mem],
        2,
        alias={5: 4},
    )
    back = across(back, C, 1)
    mine, other = total(send, keep)
    table, state = call(
        last_entities,
        "svhhh",
        [("h", grown), ("v", shape(1, ROWS))],
        (counts, state, store, back, edges),
        [table_mem, table_mem, back_mem, edge_mem],
        4,
        63 << 20,
    )
    rel, rel_state = call(
        last_relations,
        "svvhv",
        [("v", shape(DIM, REL)), ("v", shape(1, REL))],
        (core, mine, other, store, rel_state),
        [flat_mem, rel_mem, rel_mem, vmem((1, RELP), F32)],
        1,
    )
    return table.T, state.reshape(ROWS), rel.T, rel_state.reshape(REL)


def solution(mesh):
    finer = Mesh(mesh.devices.reshape(8, 4, 4, 2), DOM)
    return jax.shard_map(
        body,
        mesh=finer,
        in_specs=(
            P(DOM, None),
            P(DOM),
            P(),
            P(),
            P(None, None, DOM),
            P(None, DOM, None),
            P(None, DOM),
        ),
        out_specs=(P(DOM, None), P(DOM), P(), P()),
        check_vma=False,
    )
```

```python
import jax
import jax.numpy as jnp
from jax import lax
from jax.experimental import pallas as pl
from jax.experimental.pallas import tpu as pltpu
from jax.sharding import Mesh
from jax.sharding import PartitionSpec as P

Z, X, Y, C = "z", "x", "y", "c"
DOM = (Z, X, Y, C)
F32 = jnp.float32
BF16 = jnp.bfloat16
RATE = 0.2

ROWS = 1024
DIM = 200
HALF = DIM // 2
LOW = 208
STACK = 2 * LOW
REL = 1345
RELP = 1408
NEG = 1000
BLOCK = 128
STEP = 256
EARLY = 256
STORE = 18
GRAD, RELATION, TABLE = 0, 1, 2
EDGES = 512
LOAD = 216
ID_ROW = 200
HIST_ROW = 208
FLAT = 2304
SIDE = FLAT // 2

VMEM = pl.BlockSpec(memory_space=pltpu.VMEM)
SMEM = pl.BlockSpec(memory_space=pltpu.SMEM)
HBM = pl.BlockSpec(memory_space=pltpu.HBM)


def shape(*dims, dtype=F32):
    return jax.ShapeDtypeStruct(dims, dtype)


def params(grant):
    return pltpu.CompilerParams(vmem_limit_bytes=grant)


def halves(value):
    high = value.astype(BF16)
    return high, (value - high.astype(F32)).astype(BF16)


def dot(a, b, dims=((1,), (0,))):
    return lax.dot_general(a, b, (dims, ((), ())), preferred_element_type=F32)


NT = ((1,), (1,))


def stack(ref, value):
    high, low = halves(value)
    gap = jnp.zeros((LOW - DIM, value.shape[1]), BF16)
    ref[0:DIM, :], ref[DIM:LOW, :] = high, gap
    ref[LOW : LOW + DIM, :], ref[LOW + DIM : STACK, :] = low, gap


def stack_dot(parts, high, low=None, dims=((1,), (0,))):
    both = dot(parts, high, dims)
    total = both[0:DIM] + both[LOW : LOW + DIM]
    return total if low is None else total + dot(parts[0:DIM], low, dims)


def one_hot(ids, count):
    places = lax.broadcasted_iota(jnp.int32, (count, ids.shape[1]), 0)
    return jnp.where(places == ids, 1.0, 0.0).astype(BF16)


def histogram(ids):
    upper = lax.broadcasted_iota(jnp.int32, (8, NEG), 0)
    lower = lax.broadcasted_iota(jnp.int32, (128, NEG), 0)
    high = jnp.where(upper == (ids >> 7), 1.0, 0.0).astype(BF16)
    low = jnp.where(lower == (ids & 127), 1.0, 0.0).astype(BF16)
    return dot(high, low, NT)


def live_sources(edges_ref, count, which):
    places = lax.broadcasted_iota(jnp.int32, (1, EDGES), 1)
    return jnp.where(places < count, edges_ref[0, which : which + 1, :], -1)


def fetch(sem, *pairs):
    copies = [pltpu.make_async_copy(a, b, sem.at[i]) for i, (a, b) in enumerate(pairs)]
    for copy in copies:
        copy.start()
    return copies


def write_lists(refs, edges_ref, negatives_ref, which):
    first = 0
    for ref in refs:
        wide = ref.shape[1]
        span = slice(first, first + wide)
        ref[ID_ROW : ID_ROW + 1, :] = edges_ref[1, which : which + 1, span].astype(F32)
        ref[ID_ROW + 1 : ID_ROW + 2, :] = edges_ref[2, which : which + 1, span].astype(F32)
        ref[ID_ROW + 2 : HIST_ROW, :] = jnp.zeros((HIST_ROW - ID_ROW - 2, wide), F32)
        for block in range(wide // BLOCK):
            k = first // BLOCK + block
            ref[HIST_ROW:LOAD, block * BLOCK : (block + 1) * BLOCK] = histogram(
                negatives_ref[which, k : k + 1, :]
            )
        first += wide


def source_rows(parts_ref, edges_ref, count, which, first, wide):
    source = live_sources(edges_ref, count, which)[:, first : first + wide]
    return stack_dot(parts_ref[...], one_hot(source, ROWS))


def prepare(
    counts_ref,
    table_hbm,
    edges_hbm,
    negatives_hbm,
    first_out,
    second_out,
    table_ref,
    edges_ref,
    negatives_ref,
    first_ref,
    second_ref,
    parts_ref,
    sem,
):
    negatives_copy, edges_copy, table_copy = fetch(
        sem, (negatives_hbm, negatives_ref), (edges_hbm, edges_ref), (table_hbm, table_ref)
    )
    negatives_copy.wait()
    edges_copy.wait()
    write_lists((first_ref, second_ref), edges_ref, negatives_ref, 0)
    table_copy.wait()
    stack(parts_ref, table_ref[...])
    count = counts_ref[0, 0]
    first_ref[0:DIM, :] = source_rows(parts_ref, edges_ref, count, 0, 0, EARLY)
    copies = fetch(sem, (first_ref, first_out))
    second_ref[0:DIM, :] = source_rows(parts_ref, edges_ref, count, 0, EARLY, EDGES - EARLY)
    copies += fetch(sem.at[1:2], (second_ref, second_out))
    for copy in copies:
        copy.wait()


def settle(table_ref, rel_ref, state_ref, store, state_out, rel_parts, table_parts, rel, sem):
    rel[:, 10 * 128 : RELP] = jnp.zeros((DIM, RELP - 10 * 128), F32)
    rel[:, 0:REL] = rel_ref[...]
    (copy,) = fetch(sem, (rel, store.at[RELATION]))
    stack(rel_parts, rel[...])
    stack(table_parts, table_ref[...])
    state_out[...] = jnp.ones((1, RELP), F32)
    state_out[:, 0:REL] = state_ref[...]
    copy.wait()


def multiply(a_re, a_im, b_re, b_im, conjugate, out, lanes):
    if conjugate:
        out[0:HALF, lanes] = a_re * b_re + a_im * b_im
        out[HALF:DIM, lanes] = a_im * b_re - a_re * b_im
    else:
        out[0:HALF, lanes] = a_re * b_re - a_im * b_im
        out[HALF:DIM, lanes] = a_re * b_im + a_im * b_re


def weights(scores, times, target, first_lane):
    small = jnp.exp(-jnp.abs(scores))
    large = 1.0 / (1.0 + small)
    small = small * large
    up = scores >= 0.0
    plus = jnp.where(up, large, small)
    minus = jnp.where(up, small, large)
    lanes = lax.broadcasted_iota(jnp.int32, (1, 128), 1) + first_lane
    return plus * times - jnp.where(lanes == target, minus, 0.0)


def edge_terms(load_ref, table_ref, rel_ref, work, sg_out, rg_ref, first, put):
    w_ref, q_ref, parts_ref, score_ref, high_ref, low_ref, back_ref = work
    wide = load_ref.shape[1]
    pick = one_hot(load_ref[ID_ROW : ID_ROW + 1, :].astype(jnp.int32), RELP)
    w_ref[...] = stack_dot(rel_ref[...], pick)
    s_re, s_im = load_ref[0:HALF, :], load_ref[HALF:DIM, :]
    w_re, w_im = w_ref[0:HALF, :], w_ref[HALF:DIM, :]
    multiply(s_re, s_im, w_re, w_im, False, q_ref, slice(None))
    product = q_ref[...]
    stack(parts_ref, product)
    target = load_ref[ID_ROW : ID_ROW + 8, :].T[:, 1:2].astype(jnp.int32)
    turned = halves(product.T)
    table_high, table_low = table_ref[0:DIM, :], table_ref[LOW : LOW + DIM, :]
    spans = [slice(start, min(start + STEP, wide)) for start in range(0, wide, STEP)]
    for edges in spans:
        count = edges.stop - edges.start
        high, low = turned[0][edges], turned[1][edges]
        both = dot(jnp.concatenate([high, low], axis=0), table_high)
        score_ref[edges, :] = both[0:count] + both[count:] + dot(high, table_low)
    table_grad = None
    for span in spans:
        for block in range(span.start, span.stop, BLOCK):
            edges = slice(block, block + BLOCK)
            for tile in range(ROWS // 128):
                lanes = slice(tile * 128, (tile + 1) * 128)
                times = load_ref[HIST_ROW + tile : HIST_ROW + tile + 1, edges] * (1.0 / NEG)
                value = weights(score_ref[edges, lanes], times, target[edges], tile * 128)
                high_ref[edges, lanes], low_ref[edges, lanes] = halves(value)
        high, low = high_ref[span, :], low_ref[span, :]
        back_ref[:, span] = stack_dot(table_ref[...], high, low, NT)
        part = stack_dot(parts_ref[:, span], high, low)
        table_grad = part if table_grad is None else table_grad + part
    copies = put(table_grad)
    up_re, up_im = back_ref[0:HALF, :], back_ref[HALF:DIM, :]
    lanes = slice(first, first + wide)
    multiply(up_re, up_im, s_re, s_im, True, rg_ref, lanes)
    multiply(up_re, up_im, w_re, w_im, True, sg_out, lanes)
    return pick, copies


def relation_grad(rg_ref, parts_ref, pick):
    stack(parts_ref, rg_ref[...])
    return stack_dot(parts_ref[...], pick, None, NT)


def split_flat(core, grad, flat, send_out, keep_out):
    for tile in range(RELP // 128):
        flat[tile * DIM : (tile + 1) * DIM, :] = grad[:, tile * 128 : (tile + 1) * 128]
    flat[RELP // 128 * DIM : FLAT, :] = jnp.zeros((FLAT - RELP // 128 * DIM, 128), F32)
    keep_out[...] = flat[pl.ds(pl.multiple_of(core * SIDE, SIDE), SIDE), :]
    send_out[...] = flat[pl.ds(pl.multiple_of((1 - core) * SIDE, SIDE), SIDE), :]


def join_flat(core, mine_ref, other_ref, flat):
    flat[pl.ds(pl.multiple_of(core * SIDE, SIDE), SIDE), :] = mine_ref[...]
    flat[pl.ds(pl.multiple_of((1 - core) * SIDE, SIDE), SIDE), :] = other_ref[...]


def adagrad(table, state, grad):
    state = state + jnp.sum(grad * grad, axis=0, keepdims=True) * (1.0 / DIM)
    return table - grad * (RATE / jnp.sqrt(state)), state


def entities_of(store, plane):
    return store.at[plane, :, 0:ROWS]


def first_piece(load_ref, table_ref, rel_ref, _, sg_out, rg_out, store, *work):
    work, grad_ref, sem = work[:-2], work[-2], work[-1]

    def put(value):
        grad_ref[...] = value
        return fetch(sem, (grad_ref, entities_of(store, GRAD)))

    _, copies = edge_terms(load_ref, table_ref, rel_ref, work, sg_out, rg_out, 0, put)
    for copy in copies:
        copy.wait()


def second_piece(
    core_ref,
    early_ref,
    load_ref,
    table_ref,
    rel_ref,
    sg_ref,
    rg_ref,
    _,
    sg_out,
    send,
    keep,
    store,
    *work,
):
    work, rg, rg_parts, flat, grad_ref, g_ref, sem = work[:-6], *work[-6:]
    (g_copy,) = fetch(sem, (entities_of(store, GRAD), g_ref))

    def put(value):
        g_copy.wait()
        grad_ref[...] = value + g_ref[...]
        return fetch(sem, (grad_ref, entities_of(store, GRAD)))

    sg_out[:, 0:EARLY] = sg_ref[...]
    rg[:, 0:EARLY] = rg_ref[...]
    pick, copies = edge_terms(load_ref, table_ref, rel_ref, work, sg_out, rg, EARLY, put)
    early = one_hot(early_ref[ID_ROW : ID_ROW + 1, :].astype(jnp.int32), RELP)
    pick = jnp.concatenate([early, pick], axis=1)
    split_flat(core_ref[0], relation_grad(rg, rg_parts, pick), flat, send, keep)
    for copy in copies:
        copy.wait()


def step_relations(core, mine_ref, other_ref, rel_ref, state_ref, flat, rel_out, state_out):
    join_flat(core, mine_ref, other_ref, flat)
    step_tiles(rel_ref, state_ref, flat, rel_out, state_out)


def step_tiles(rel_ref, state_ref, flat, rel_out, state_out):
    for tile in range(RELP // 128):
        lanes = slice(tile * 128, (tile + 1) * 128)
        rel_out[:, lanes], state_out[:, lanes] = adagrad(
            rel_ref[:, lanes], state_ref[:, lanes], flat[tile * DIM : (tile + 1) * DIM, :]
        )


def second_round(
    core_ref,
    mine_ref,
    other_ref,
    state_ref,
    load_ref,
    _,
    sg_out,
    send,
    keep,
    state_out,
    store,
    *work,
):
    work, rg, rg_parts, flat, old_ref, rel_ref, grad_ref, tables, rels, sem = work[:-9], *work[-9:]
    rel_copy, table_copy = fetch(
        sem, (store.at[RELATION], old_ref), (entities_of(store, TABLE), grad_ref)
    )
    core = core_ref[0]
    rel_copy.wait()
    step_relations(core, mine_ref, other_ref, old_ref, state_ref, flat, rel_ref, state_out)
    (rel_copy,) = fetch(sem, (rel_ref, store.at[RELATION]))
    table_copy.wait()
    stack(tables, grad_ref[...])

    def put(value):
        grad_ref[...] = value
        return fetch(sem.at[1:2], (grad_ref, entities_of(store, GRAD)))

    stack(rels, rel_ref[...])
    pick, copies = edge_terms(load_ref, tables, rels, work, sg_out, rg, 0, put)
    split_flat(core, relation_grad(rg, rg_parts, pick), flat, send, keep)
    for copy in [rel_copy, *copies]:
        copy.wait()


def step_entities(
    table_ref, state_ref, grad_ref, back_ref, parts_ref, edges_ref, count, which
):
    pick = one_hot(live_sources(edges_ref, count, which), ROWS)
    stack(parts_ref, back_ref[...])
    grad = grad_ref[...] + stack_dot(parts_ref[...], pick, None, NT)
    return adagrad(table_ref[...], state_ref[...], grad)


def between(
    counts_ref,
    table_hbm,
    state_ref,
    _,
    back_hbm,
    edges_hbm,
    negatives_hbm,
    state_out,
    store,
    load,
    table_ref,
    grad_ref,
    back_ref,
    edges_ref,
    negatives_ref,
    parts_ref,
    tables_ref,
    sem,
):
    copies = fetch(
        sem,
        (edges_hbm, edges_ref),
        (back_hbm, back_ref),
        (entities_of(store, GRAD), grad_ref),
        (table_hbm, table_ref),
        (negatives_hbm, negatives_ref),
    )
    for copy in copies:
        copy.wait()
    table, state_out[...] = step_entities(
        table_ref, state_ref, grad_ref, back_ref, parts_ref, edges_ref, counts_ref[0, 0], 0
    )
    table_ref[...] = table
    (copy,) = fetch(sem, (table_ref, entities_of(store, TABLE)))
    stack(tables_ref, table)
    write_lists((load,), edges_ref, negatives_ref, 1)
    load[0:DIM, :] = source_rows(tables_ref, edges_ref, counts_ref[0, 1], 1, 0, EDGES)
    copy.wait()


def last_entities(
    counts_ref,
    state_ref,
    store,
    back_hbm,
    edges_hbm,
    table_out,
    state_out,
    table_ref,
    grad_ref,
    back_ref,
    edges_ref,
    parts_ref,
    sem,
):
    copies = fetch(
        sem,
        (edges_hbm, edges_ref),
        (back_hbm, back_ref),
        (entities_of(store, GRAD), grad_ref),
        (entities_of(store, TABLE), table_ref),
    )
    for copy in copies:
        copy.wait()
    table, state_out[...] = step_entities(
        table_ref, state_ref, grad_ref, back_ref, parts_ref, edges_ref, counts_ref[0, 1], 1
    )
    table_ref[...] = table
    (copy,) = fetch(sem, (table_ref, table_out))
    copy.wait()


def last_relations(
    core_ref,
    mine_ref,
    other_ref,
    store,
    state_ref,
    rel_out,
    state_out,
    flat,
    old_ref,
    rel,
    state,
    sem,
):
    (copy,) = fetch(sem, (store.at[RELATION], old_ref))
    join_flat(core_ref[0], mine_ref, other_ref, flat)
    copy.wait()
    step_tiles(old_ref, state_ref, flat, rel, state)
    rel_out[...] = rel[:, 0:REL]
    state_out[...] = state[0, 0:REL]


def work_shapes(wide):
    return [
        pltpu.VMEM((DIM, wide), F32),
        pltpu.VMEM((DIM, wide), F32),
        pltpu.VMEM((STACK, wide), BF16),
        pltpu.VMEM((wide, ROWS), F32),
        pltpu.VMEM((wide, ROWS), BF16),
        pltpu.VMEM((wide, ROWS), BF16),
        pltpu.VMEM((DIM, wide), F32),
    ]


SPECS = {"s": SMEM, "v": VMEM, "h": HBM}


def call(body, ins, outs, operands, scratch=(), copies=0, grant=48 << 20, alias=None):
    scratch = list(scratch) + ([pltpu.SemaphoreType.DMA((copies,))] if copies else [])
    return pl.pallas_call(
        body,
        out_shape=[out for _, out in outs],
        in_specs=[SPECS[kind] for kind in ins],
        out_specs=[SPECS[kind] for kind, _ in outs],
        scratch_shapes=scratch,
        input_output_aliases=alias or {},
        compiler_params=params(grant),
    )(*operands)


def across(value, axis, apart):
    count = lax.axis_size(axis)
    return lax.ppermute(value, axis, [(i, i ^ apart) for i in range(count)])


def total(send, keep):
    part = (keep + across(send, C, 1)).reshape(16, SIDE // 16, 128)
    part = lax.all_to_all(part, (Y, X), 0, 0, tiled=True).sum(axis=0)
    part = jnp.broadcast_to(part[None], (8, *part.shape))
    part = lax.all_to_all(part, Z, 0, 0, tiled=True).sum(axis=0)
    part = jnp.broadcast_to(part[None], (16, *part.shape))
    part = lax.all_to_all(part, (Y, X), 0, 0, tiled=True)
    mine = part.reshape(SIDE, 128)
    return mine, across(mine, C, 1)


def body(entities, entity_state, relations, relation_state, edges, negatives, counts):
    core = lax.axis_index(C).astype(jnp.int32).reshape(1)
    table, rel, counts = entities.T, relations.T, counts.T
    edges = edges.transpose(1, 0, 2)
    state = entity_state.reshape(1, ROWS)
    late = EDGES - EARLY
    grown = shape(DIM, ROWS)
    vmem = pltpu.VMEM
    table_mem, rg_mem = vmem((DIM, ROWS), F32), vmem((STACK, EDGES), BF16)
    tables_mem, rels_mem = vmem((STACK, ROWS), BF16), vmem((STACK, RELP), BF16)
    flat_mem = vmem((FLAT, 128), F32)
    back_mem, rel_mem = vmem((DIM, EDGES), F32), vmem((DIM, RELP), F32)
    edge_mem, negative_mem = vmem((3, 2, EDGES), jnp.int32), vmem(negatives.shape, jnp.int32)
    first, second = call(
        prepare,
        "shhh",
        [("h", shape(LOAD, EARLY)), ("h", shape(LOAD, late))],
        (counts, table, edges, negatives),
        [table_mem, edge_mem, negative_mem, vmem((LOAD, EARLY), F32), vmem((LOAD, late), F32)]
        + [tables_mem],
        3,
        63 << 20,
    )
    first = across(first, Z, 4)
    second = across(second, Z, 4)
    store_out = ("h", shape(STORE, DIM, RELP))
    store, rel_state, rel_parts, table_parts = call(
        settle,
        "vvv",
        [store_out, ("v", shape(1, RELP))]
        + [("v", shape(STACK, RELP, dtype=BF16)), ("v", shape(STACK, ROWS, dtype=BF16))],
        (table, rel, relation_state.reshape(1, REL)),
        [rel_mem],
        1,
    )
    piece = ("v", shape(DIM, EARLY))
    back, rel_terms, store = call(
        first_piece,
        "vvvh",
        [piece, piece, store_out],
        (first, table_parts, rel_parts, store),
        work_shapes(EARLY) + [table_mem],
        1,
        alias={3: 2},
    )
    half = ("v", shape(SIDE, 128))
    back, send, keep, store = call(
        second_piece,
        "svvvvvvh",
        [("v", shape(DIM, EDGES)), half, half, store_out],
        (core, first, second, table_parts, rel_parts, back, rel_terms, store),
        work_shapes(late) + [back_mem, rg_mem, flat_mem, table_mem, table_mem],
        1,
        alias={7: 3},
    )
    back = across(back, Z, 4)
    mine, other = total(send, keep)
    state, store, load = call(
        between,
        "shvhhhh",
        [("v", shape(1, ROWS)), store_out, ("v", shape(LOAD, EDGES))],
        (counts, table, state, store, back, edges, negatives),
        [table_mem, table_mem, back_mem, edge_mem, negative_mem, rg_mem, tables_mem],
        5,
        63 << 20,
        {3: 1},
    )
    load = across(load, C, 1)
    back, send, keep, rel_state, store = call(
        second_round,
        "svvvvh",
        [("v", shape(DIM, EDGES)), half, half, ("v", shape(1, RELP)), store_out],
        (core, mine, other, rel_state, load, store),
        work_shapes(EDGES)
        + [back_mem, rg_mem, flat_mem, rel_mem, rel_mem, table_mem, tables_mem, rels_mem],
        2,
        alias={5: 4},
    )
    back = across(back, C, 1)
    mine, other = total(send, keep)
    table, state = call(
        last_entities,
        "svhhh",
        [("h", grown), ("v", shape(1, ROWS))],
        (counts, state, store, back, edges),
        [table_mem, table_mem, back_mem, edge_mem, rg_mem],
        4,
        63 << 20,
    )
    rel, rel_state = call(
        last_relations,
        "svvhv",
        [("v", shape(DIM, REL)), ("v", shape(REL))],
        (core, mine, other, store, rel_state),
        [flat_mem, rel_mem, rel_mem, vmem((1, RELP), F32)],
        1,
    )
    return table.T, state.reshape(ROWS), rel.T, rel_state


def solution(mesh):
    finer = Mesh(mesh.devices.reshape(8, 4, 4, 2), DOM)
    return jax.shard_map(
        body,
        mesh=finer,
        in_specs=(
            P(DOM, None),
            P(DOM),
            P(),
            P(),
            P(None, None, DOM),
            P(None, DOM, None),
            P(None, DOM),
        ),
        out_specs=(P(DOM, None), P(DOM), P(), P()),
        check_vma=False,
    )
```

```python
import jax
import jax.numpy as jnp
from jax import lax
from jax.experimental import pallas as pl
from jax.experimental.pallas import tpu as pltpu
from jax.sharding import Mesh
from jax.sharding import PartitionSpec as P

Z, X, Y, C = "z", "x", "y", "c"
DOM = (Z, X, Y, C)
F32 = jnp.float32
BF16 = jnp.bfloat16
RATE = 0.2

ROWS = 1024
DIM = 200
HALF = DIM // 2
LOW = 208
STACK = 2 * LOW
REL = 1345
RELP = 1408
NEG = 1000
BLOCK = 128
STEP = 256
EARLY = 256
STORE = 18
GRAD, RELATION, TABLE = 0, 1, 2
EDGES = 512
LOAD = 216
ID_ROW = 200
HIST_ROW = 208
FLAT = 2304
SIDE = FLAT // 2

VMEM = pl.BlockSpec(memory_space=pltpu.VMEM)
SMEM = pl.BlockSpec(memory_space=pltpu.SMEM)
HBM = pl.BlockSpec(memory_space=pltpu.HBM)


def shape(*dims, dtype=F32):
    return jax.ShapeDtypeStruct(dims, dtype)


def params(grant):
    return pltpu.CompilerParams(vmem_limit_bytes=grant)


def halves(value):
    high = value.astype(BF16)
    return high, (value - high.astype(F32)).astype(BF16)


def dot(a, b, dims=((1,), (0,))):
    return lax.dot_general(a, b, (dims, ((), ())), preferred_element_type=F32)


NT = ((1,), (1,))


def dot3(a, b, dims=((1,), (0,))):
    return dot(a[0], b[0], dims) + (dot(a[1], b[0], dims) + dot(a[0], b[1], dims))


def stack(ref, value):
    high, low = halves(value)
    gap = jnp.zeros((LOW - DIM, value.shape[1]), BF16)
    ref[0:DIM, :], ref[DIM:LOW, :] = high, gap
    ref[LOW : LOW + DIM, :], ref[LOW + DIM : STACK, :] = low, gap


def stack_dot(parts, high, low=None, dims=((1,), (0,))):
    both = dot(parts, high, dims)
    total = both[0:DIM] + both[LOW : LOW + DIM]
    return total if low is None else total + dot(parts[0:DIM], low, dims)


def one_hot(ids, count):
    places = lax.broadcasted_iota(jnp.int32, (count, ids.shape[1]), 0)
    return jnp.where(places == ids, 1.0, 0.0).astype(BF16)


def histogram(ids):
    upper = lax.broadcasted_iota(jnp.int32, (8, NEG), 0)
    lower = lax.broadcasted_iota(jnp.int32, (128, NEG), 0)
    high = jnp.where(upper == (ids >> 7), 1.0, 0.0).astype(BF16)
    low = jnp.where(lower == (ids & 127), 1.0, 0.0).astype(BF16)
    return dot(high, low, NT)


def live_sources(edges_ref, count, which):
    places = lax.broadcasted_iota(jnp.int32, (1, EDGES), 1)
    return jnp.where(places < count, edges_ref[0, which : which + 1, :], -1)


def fetch(sem, *pairs):
    copies = [pltpu.make_async_copy(a, b, sem.at[i]) for i, (a, b) in enumerate(pairs)]
    for copy in copies:
        copy.start()
    return copies


def write_lists(refs, edges_ref, negatives_ref, which):
    first = 0
    for ref in refs:
        wide = ref.shape[1]
        span = slice(first, first + wide)
        ref[ID_ROW : ID_ROW + 1, :] = edges_ref[1, which : which + 1, span].astype(F32)
        ref[ID_ROW + 1 : ID_ROW + 2, :] = edges_ref[2, which : which + 1, span].astype(F32)
        ref[ID_ROW + 2 : HIST_ROW, :] = jnp.zeros((HIST_ROW - ID_ROW - 2, wide), F32)
        for block in range(wide // BLOCK):
            k = first // BLOCK + block
            ref[HIST_ROW:LOAD, block * BLOCK : (block + 1) * BLOCK] = histogram(
                negatives_ref[which, k : k + 1, :]
            )
        first += wide


def source_rows(parts_ref, edges_ref, count, which, first, wide):
    source = live_sources(edges_ref, count, which)[:, first : first + wide]
    return stack_dot(parts_ref[...], one_hot(source, ROWS))


def prepare(
    counts_ref,
    table_hbm,
    edges_hbm,
    negatives_hbm,
    first_out,
    second_out,
    table_ref,
    edges_ref,
    negatives_ref,
    first_ref,
    second_ref,
    parts_ref,
    sem,
):
    negatives_copy, edges_copy, table_copy = fetch(
        sem, (negatives_hbm, negatives_ref), (edges_hbm, edges_ref), (table_hbm, table_ref)
    )
    negatives_copy.wait()
    edges_copy.wait()
    write_lists((first_ref, second_ref), edges_ref, negatives_ref, 0)
    table_copy.wait()
    stack(parts_ref, table_ref[...])
    count = counts_ref[0, 0]
    first_ref[0:DIM, :] = source_rows(parts_ref, edges_ref, count, 0, 0, EARLY)
    copies = fetch(sem, (first_ref, first_out))
    second_ref[0:DIM, :] = source_rows(parts_ref, edges_ref, count, 0, EARLY, EDGES - EARLY)
    copies += fetch(sem.at[1:2], (second_ref, second_out))
    for copy in copies:
        copy.wait()


def settle(
    table_ref,
    rel_ref,
    state_ref,
    store,
    state_out,
    rel_high,
    rel_low,
    table_high,
    table_low,
    rel,
    sem,
):
    rel[:, 10 * 128 : RELP] = jnp.zeros((DIM, RELP - 10 * 128), F32)
    rel[:, 0:REL] = rel_ref[...]
    (copy,) = fetch(sem, (rel, store.at[RELATION]))
    rel_high[...], rel_low[...] = halves(rel[...])
    table_high[...], table_low[...] = halves(table_ref[...])
    state_out[...] = jnp.ones((1, RELP), F32)
    state_out[:, 0:REL] = state_ref[...]
    copy.wait()


def multiply(a_re, a_im, b_re, b_im, conjugate, out, lanes):
    if conjugate:
        out[0:HALF, lanes] = a_re * b_re + a_im * b_im
        out[HALF:DIM, lanes] = a_im * b_re - a_re * b_im
    else:
        out[0:HALF, lanes] = a_re * b_re - a_im * b_im
        out[HALF:DIM, lanes] = a_re * b_im + a_im * b_re


def weights(scores, times, target, first_lane):
    small = jnp.exp(-jnp.abs(scores))
    large = 1.0 / (1.0 + small)
    small = small * large
    up = scores >= 0.0
    plus = jnp.where(up, large, small)
    minus = jnp.where(up, small, large)
    lanes = lax.broadcasted_iota(jnp.int32, (1, 128), 1) + first_lane
    return plus * times - jnp.where(lanes == target, minus, 0.0)


def edge_terms(load_ref, table_parts, rel_parts, work, sg_out, rg_ref, first, put):
    w_ref, q_ref, score_ref, high_ref, low_ref, back_ref = work
    wide = load_ref.shape[1]
    pick = one_hot(load_ref[ID_ROW : ID_ROW + 1, :].astype(jnp.int32), RELP)
    w_ref[...] = dot(rel_parts[0], pick) + dot(rel_parts[1], pick)
    s_re, s_im = load_ref[0:HALF, :], load_ref[HALF:DIM, :]
    w_re, w_im = w_ref[0:HALF, :], w_ref[HALF:DIM, :]
    multiply(s_re, s_im, w_re, w_im, False, q_ref, slice(None))
    product = q_ref[...]
    product_parts = halves(product)
    target = load_ref[ID_ROW : ID_ROW + 8, :].T[:, 1:2].astype(jnp.int32)
    turned = halves(product.T)
    spans = [slice(start, min(start + STEP, wide)) for start in range(0, wide, STEP)]
    for edges in spans:
        score_ref[edges, :] = dot3((turned[0][edges], turned[1][edges]), table_parts)
    table_grad = None
    for span in spans:
        for block in range(span.start, span.stop, BLOCK):
            edges = slice(block, block + BLOCK)
            for tile in range(ROWS // 128):
                lanes = slice(tile * 128, (tile + 1) * 128)
                times = load_ref[HIST_ROW + tile : HIST_ROW + tile + 1, edges] * (1.0 / NEG)
                value = weights(score_ref[edges, lanes], times, target[edges], tile * 128)
                high_ref[edges, lanes], low_ref[edges, lanes] = halves(value)
        weight_parts = high_ref[span, :], low_ref[span, :]
        back_ref[:, span] = dot3(table_parts, weight_parts, NT)
        part = dot3((product_parts[0][:, span], product_parts[1][:, span]), weight_parts)
        table_grad = part if table_grad is None else table_grad + part
    copies = put(table_grad)
    up_re, up_im = back_ref[0:HALF, :], back_ref[HALF:DIM, :]
    lanes = slice(first, first + wide)
    multiply(up_re, up_im, s_re, s_im, True, rg_ref, lanes)
    multiply(up_re, up_im, w_re, w_im, True, sg_out, lanes)
    return pick, copies


def relation_grad(rg_ref, pick):
    high, low = halves(rg_ref[...])
    return dot(high, pick, NT) + dot(low, pick, NT)


def split_flat(core, grad, flat, send_out, keep_out):
    for tile in range(RELP // 128):
        flat[tile * DIM : (tile + 1) * DIM, :] = grad[:, tile * 128 : (tile + 1) * 128]
    flat[RELP // 128 * DIM : FLAT, :] = jnp.zeros((FLAT - RELP // 128 * DIM, 128), F32)
    keep_out[...] = flat[pl.ds(pl.multiple_of(core * SIDE, SIDE), SIDE), :]
    send_out[...] = flat[pl.ds(pl.multiple_of((1 - core) * SIDE, SIDE), SIDE), :]


def join_flat(core, mine_ref, other_ref, flat):
    flat[pl.ds(pl.multiple_of(core * SIDE, SIDE), SIDE), :] = mine_ref[...]
    flat[pl.ds(pl.multiple_of((1 - core) * SIDE, SIDE), SIDE), :] = other_ref[...]


def adagrad(table, state, grad):
    state = state + jnp.sum(grad * grad, axis=0, keepdims=True) * (1.0 / DIM)
    return table - grad * (RATE / jnp.sqrt(state)), state


def entities_of(store, plane):
    return store.at[plane, :, 0:ROWS]


def first_piece(
    load_ref, high_ref, low_ref, rel_high, rel_low, _, sg_out, rg_out, store, *work
):
    work, grad_ref, sem = work[:-2], work[-2], work[-1]

    def put(value):
        grad_ref[...] = value
        return fetch(sem, (grad_ref, entities_of(store, GRAD)))

    table_parts, rel_parts = (high_ref[...], low_ref[...]), (rel_high[...], rel_low[...])
    _, copies = edge_terms(load_ref, table_parts, rel_parts, work, sg_out, rg_out, 0, put)
    for copy in copies:
        copy.wait()


def second_piece(
    core_ref,
    early_ref,
    load_ref,
    high_ref,
    low_ref,
    rel_high,
    rel_low,
    sg_ref,
    rg_ref,
    _,
    sg_out,
    send,
    keep,
    store,
    *work,
):
    work, rg, flat, grad_ref, g_ref, sem = work[:-5], *work[-5:]
    (g_copy,) = fetch(sem, (entities_of(store, GRAD), g_ref))

    def put(value):
        g_copy.wait()
        grad_ref[...] = value + g_ref[...]
        return fetch(sem, (grad_ref, entities_of(store, GRAD)))

    table_parts, rel_parts = (high_ref[...], low_ref[...]), (rel_high[...], rel_low[...])
    sg_out[:, 0:EARLY] = sg_ref[...]
    rg[:, 0:EARLY] = rg_ref[...]
    pick, copies = edge_terms(load_ref, table_parts, rel_parts, work, sg_out, rg, EARLY, put)
    early = one_hot(early_ref[ID_ROW : ID_ROW + 1, :].astype(jnp.int32), RELP)
    pick = jnp.concatenate([early, pick], axis=1)
    split_flat(core_ref[0], relation_grad(rg, pick), flat, send, keep)
    for copy in copies:
        copy.wait()


def step_tiles(rel_ref, state_ref, flat, rel_out, state_out):
    for tile in range(RELP // 128):
        lanes = slice(tile * 128, (tile + 1) * 128)
        rel_out[:, lanes], state_out[:, lanes] = adagrad(
            rel_ref[:, lanes], state_ref[:, lanes], flat[tile * DIM : (tile + 1) * DIM, :]
        )


def second_round(
    core_ref,
    mine_ref,
    other_ref,
    state_ref,
    load_ref,
    _,
    sg_out,
    send,
    keep,
    state_out,
    store,
    *work,
):
    work, rg, flat, old_ref, rel_ref, grad_ref, sem = work[:-6], *work[-6:]
    rel_copy, table_copy = fetch(
        sem, (store.at[RELATION], old_ref), (entities_of(store, TABLE), grad_ref)
    )
    core = core_ref[0]
    join_flat(core, mine_ref, other_ref, flat)
    rel_copy.wait()
    step_tiles(old_ref, state_ref, flat, rel_ref, state_out)
    table_copy.wait()
    table_parts = halves(grad_ref[...])
    (rel_copy,) = fetch(sem, (rel_ref, store.at[RELATION]))

    def put(value):
        grad_ref[...] = value
        return fetch(sem.at[1:2], (grad_ref, entities_of(store, GRAD)))

    rel_parts = halves(rel_ref[...])
    pick, copies = edge_terms(load_ref, table_parts, rel_parts, work, sg_out, rg, 0, put)
    split_flat(core, relation_grad(rg, pick), flat, send, keep)
    for copy in [rel_copy, *copies]:
        copy.wait()


def step_entities(
    table_ref, state_ref, grad_ref, back_ref, parts_ref, edges_ref, count, which
):
    pick = one_hot(live_sources(edges_ref, count, which), ROWS)
    stack(parts_ref, back_ref[...])
    grad = grad_ref[...] + stack_dot(parts_ref[...], pick, None, NT)
    return adagrad(table_ref[...], state_ref[...], grad)


def between(
    counts_ref,
    table_hbm,
    state_ref,
    _,
    back_hbm,
    edges_hbm,
    negatives_hbm,
    state_out,
    store,
    load,
    table_ref,
    grad_ref,
    back_ref,
    edges_ref,
    negatives_ref,
    parts_ref,
    tables_ref,
    sem,
):
    copies = fetch(
        sem,
        (edges_hbm, edges_ref),
        (back_hbm, back_ref),
        (entities_of(store, GRAD), grad_ref),
        (table_hbm, table_ref),
        (negatives_hbm, negatives_ref),
    )
    for copy in copies:
        copy.wait()
    table, state_out[...] = step_entities(
        table_ref, state_ref, grad_ref, back_ref, parts_ref, edges_ref, counts_ref[0, 0], 0
    )
    table_ref[...] = table
    (copy,) = fetch(sem, (table_ref, entities_of(store, TABLE)))
    stack(tables_ref, table)
    write_lists((load,), edges_ref, negatives_ref, 1)
    load[0:DIM, :] = source_rows(tables_ref, edges_ref, counts_ref[0, 1], 1, 0, EDGES)
    copy.wait()


def last_entities(
    counts_ref,
    state_ref,
    store,
    back_hbm,
    edges_hbm,
    table_out,
    state_out,
    table_ref,
    grad_ref,
    back_ref,
    edges_ref,
    parts_ref,
    sem,
):
    copies = fetch(
        sem,
        (edges_hbm, edges_ref),
        (back_hbm, back_ref),
        (entities_of(store, GRAD), grad_ref),
        (entities_of(store, TABLE), table_ref),
    )
    for copy in copies:
        copy.wait()
    table, state_out[...] = step_entities(
        table_ref, state_ref, grad_ref, back_ref, parts_ref, edges_ref, counts_ref[0, 1], 1
    )
    table_ref[...] = table
    (copy,) = fetch(sem, (table_ref, table_out))
    copy.wait()


def last_relations(
    core_ref,
    mine_ref,
    other_ref,
    store,
    state_ref,
    rel_out,
    state_out,
    flat,
    old_ref,
    rel,
    state,
    sem,
):
    (copy,) = fetch(sem, (store.at[RELATION], old_ref))
    join_flat(core_ref[0], mine_ref, other_ref, flat)
    copy.wait()
    step_tiles(old_ref, state_ref, flat, rel, state)
    rel_out[...] = rel[:, 0:REL]
    state_out[...] = state[0, 0:REL]


def work_shapes(wide):
    return [
        pltpu.VMEM((DIM, wide), F32),
        pltpu.VMEM((DIM, wide), F32),
        pltpu.VMEM((wide, ROWS), F32),
        pltpu.VMEM((wide, ROWS), BF16),
        pltpu.VMEM((wide, ROWS), BF16),
        pltpu.VMEM((DIM, wide), F32),
    ]


SPECS = {"s": SMEM, "v": VMEM, "h": HBM}


def call(body, ins, outs, operands, scratch=(), copies=0, grant=48 << 20, alias=None):
    scratch = list(scratch) + ([pltpu.SemaphoreType.DMA((copies,))] if copies else [])
    return pl.pallas_call(
        body,
        out_shape=[out for _, out in outs],
        in_specs=[SPECS[kind] for kind in ins],
        out_specs=[SPECS[kind] for kind, _ in outs],
        scratch_shapes=scratch,
        input_output_aliases=alias or {},
        compiler_params=params(grant),
    )(*operands)


def across(value, axis, apart):
    count = lax.axis_size(axis)
    return lax.ppermute(value, axis, [(i, i ^ apart) for i in range(count)])


def total(send, keep):
    part = (keep + across(send, C, 1)).reshape(16, SIDE // 16, 128)
    part = lax.all_to_all(part, (Y, X), 0, 0, tiled=True).sum(axis=0)
    part = jnp.broadcast_to(part[None], (8, *part.shape))
    part = lax.all_to_all(part, Z, 0, 0, tiled=True).sum(axis=0)
    part = jnp.broadcast_to(part[None], (16, *part.shape))
    part = lax.all_to_all(part, (Y, X), 0, 0, tiled=True)
    mine = part.reshape(SIDE, 128)
    return mine, across(mine, C, 1)


def body(entities, entity_state, relations, relation_state, edges, negatives, counts):
    core = lax.axis_index(C).astype(jnp.int32).reshape(1)
    table, rel, counts = entities.T, relations.T, counts.T
    edges = edges.transpose(1, 0, 2)
    state = entity_state.reshape(1, ROWS)
    late = EDGES - EARLY
    grown = shape(DIM, ROWS)
    narrow = shape(DIM, ROWS, dtype=BF16)
    wide_rel = shape(DIM, RELP, dtype=BF16)
    vmem = pltpu.VMEM
    table_mem, back_parts_mem = vmem((DIM, ROWS), F32), vmem((STACK, EDGES), BF16)
    parts_mem = vmem((STACK, ROWS), BF16)
    flat_mem = vmem((FLAT, 128), F32)
    back_mem, rel_mem = vmem((DIM, EDGES), F32), vmem((DIM, RELP), F32)
    edge_mem, negative_mem = vmem((3, 2, EDGES), jnp.int32), vmem(negatives.shape, jnp.int32)
    first, second = call(
        prepare,
        "shhh",
        [("h", shape(LOAD, EARLY)), ("h", shape(LOAD, late))],
        (counts, table, edges, negatives),
        [table_mem, edge_mem, negative_mem, vmem((LOAD, EARLY), F32), vmem((LOAD, late), F32)]
        + [parts_mem],
        3,
        63 << 20,
    )
    first = across(first, Z, 4)
    second = across(second, Z, 4)
    store_out = ("h", shape(STORE, DIM, RELP))
    store, rel_state, rel_high, rel_low, high, low = call(
        settle,
        "vvv",
        [store_out, ("v", shape(1, RELP))] + [("v", wide_rel)] * 2 + [("v", narrow)] * 2,
        (table, rel, relation_state.reshape(1, REL)),
        [rel_mem],
        1,
    )
    piece = ("v", shape(DIM, EARLY))
    back, rel_terms, store = call(
        first_piece,
        "vvvvvh",
        [piece, piece, store_out],
        (first, high, low, rel_high, rel_low, store),
        work_shapes(EARLY) + [table_mem],
        1,
        alias={5: 2},
    )
    half = ("v", shape(SIDE, 128))
    back, send, keep, store = call(
        second_piece,
        "svvvvvvvvh",
        [("v", shape(DIM, EDGES)), half, half, store_out],
        (core, first, second, high, low, rel_high, rel_low, back, rel_terms, store),
        work_shapes(late) + [back_mem, flat_mem, table_mem, table_mem],
        1,
        alias={9: 3},
    )
    back = across(back, Z, 4)
    mine, other = total(send, keep)
    state, store, load = call(
        between,
        "shvhhhh",
        [("v", shape(1, ROWS)), store_out, ("v", shape(LOAD, EDGES))],
        (counts, table, state, store, back, edges, negatives),
        [table_mem, table_mem, back_mem, edge_mem, negative_mem, back_parts_mem, parts_mem],
        5,
        63 << 20,
        {3: 1},
    )
    load = across(load, C, 1)
    back, send, keep, rel_state, store = call(
        second_round,
        "svvvvh",
        [("v", shape(DIM, EDGES)), half, half, ("v", shape(1, RELP)), store_out],
        (core, mine, other, rel_state, load, store),
        work_shapes(EDGES)
        + [back_mem, flat_mem, rel_mem, rel_mem, table_mem],
        2,
        alias={5: 4},
    )
    back = across(back, C, 1)
    mine, other = total(send, keep)
    table, state = call(
        last_entities,
        "svhhh",
        [("h", grown), ("v", shape(1, ROWS))],
        (counts, state, store, back, edges),
        [table_mem, table_mem, back_mem, edge_mem, back_parts_mem],
        4,
        63 << 20,
    )
    rel, rel_state = call(
        last_relations,
        "svvhv",
        [("v", shape(DIM, REL)), ("v", shape(REL))],
        (core, mine, other, store, rel_state),
        [flat_mem, rel_mem, rel_mem, vmem((1, RELP), F32)],
        1,
    )
    return table.T, state.reshape(ROWS), rel.T, rel_state


def solution(mesh):
    finer = Mesh(mesh.devices.reshape(8, 4, 4, 2), DOM)
    return jax.shard_map(
        body,
        mesh=finer,
        in_specs=(
            P(DOM, None),
            P(DOM),
            P(),
            P(),
            P(None, None, DOM),
            P(None, DOM, None),
            P(None, DOM),
        ),
        out_specs=(P(DOM, None), P(DOM), P(), P()),
        check_vma=False,
    )
```
